8 devices in a mesh: batch: 1 (over z), row: 8 (over y, x, core).
Axes of the slice: x: 2, y: 2, z: 1, core: 2. Of those that a mesh axis runs over, the one named last changes fastest.
Arguments:
- trans_mat: bfloat16 [16384, 16384], P(('batch', 'row'))
- teleport: float32 [16384, 256], P(('batch', 'row'))
- dangling: int32 [16384], P(('batch', 'row'))
- damping: float32 [8], replicated
- rank_init: float32 [16384, 256], P(('batch', 'row'))
Outputs:
- output: float32 [16384, 256], P(('batch', 'row'))
All inputs are finite; a program needn't handle non-finite values.
Results may differ from the reference program's by a relative error of at most 0.001.
Values are sent between devices in bfloat16 or wider.
A program may use at most 1 GiB of HBM per device.

```python
import jax
import jax.numpy as jnp
from jax import lax

NODES = 16384
SEEDS = 256
SWEEPS = 8


def setup_inputs(seed: int = 0, part: int = 0) -> dict:
    base_key = jax.random.key(seed)
    part_key = jax.random.fold_in(base_key, part)
    key_list = jax.random.split(part_key, 8)
    dangling = (jax.random.randint(key_list[0], (NODES,), 0, 100) < 20).astype(jnp.int32)
    popular = jnp.exp(0.8 * jax.random.normal(key_list[1], (NODES,), jnp.float32))
    weights = popular[:, None] * jnp.maximum(jax.random.uniform(key_list[2], (NODES, NODES), jnp.float32) - 0.5, 0.0)
    keep_cols = 1.0 - dangling.astype(jnp.float32)
    col_sum = jnp.sum(weights, axis=0)
    trans_mat = (weights * (keep_cols / jnp.maximum(col_sum, 1e-6))[None, :]).astype(jnp.bfloat16)
    tele_raw = jnp.exp(1.2 * jax.random.normal(key_list[3], (NODES, SEEDS), jnp.float32))
    teleport = tele_raw / jnp.mean(tele_raw, axis=0, keepdims=True)
    col_scale = jax.random.uniform(key_list[4], (1, SEEDS), jnp.float32, 0.3, 3.0)
    rank_init = col_scale * jax.random.uniform(key_list[5], (NODES, SEEDS), jnp.float32, 0.2, 1.8)
    damping = jax.random.uniform(jax.random.key(seed + 1), (SWEEPS,), jnp.float32, 0.75, 0.95)
    return {"trans_mat": trans_mat, "teleport": teleport, "dangling": dangling, "damping": damping, "rank_init": rank_init}


def reference(trans_mat, teleport, dangling, damping, rank_init):
    dang_float = dangling.astype(jnp.float32)

    def one_sweep(rank_cur, factor):
        prod_rows = jnp.dot(trans_mat, rank_cur.astype(jnp.bfloat16), preferred_element_type=jnp.float32)
        dang_mass = jnp.dot(dang_float, rank_cur, preferred_element_type=jnp.float32)
        rank_next = factor * prod_rows + (1.0 - factor) * teleport + (factor / NODES) * dang_mass[None, :]
        return rank_next, None

    rank_final, unused = lax.scan(one_sweep, rank_init, damping)
    return rank_final
```

```python
import functools

import jax
import jax.numpy as jnp
from jax import lax
from jax.experimental import pallas as pl
from jax.experimental.pallas import tpu as pltpu
from jax.sharding import PartitionSpec as P

MESH = pl.DeviceIdType.MESH

DEV = 8
ROWS = 2048
TILE = 512
HALF = 128
COLS = 256
KEEP = 14
RING = 6
CHUNKS = 32
MROWS = 1024

X_SLOTS = ((0, 0, 0), (0, 1, 0), (0, 0, 1), (0, 1, 1), (1, 2, 0), (1, 2, 1), (0, 2, 0), (0, 2, 1), (1, 3, 0), (1, 3, 1), (0, 3, 0), (0, 3, 1))
Y_SLOTS = ((0, 2, 0), (0, 3, 0), (0, 2, 1), (0, 3, 1), (1, 0, 0), (1, 0, 1), (0, 0, 0), (0, 0, 1), (1, 1, 0), (1, 1, 1), (0, 1, 0), (0, 1, 1))


def kernel(sweeps, mat, tele, dang, damp, start, out, rbuf, abuf, acc, tbuf, dcol, draw, mbuf, asem, lsem, ssem, xsem, ysem, dsem, msend, mrecv, osem):
    me = lax.axis_index("row")
    core = lax.rem(me, 2)
    xbit = lax.rem(lax.div(me, 2), 2)
    ybit = lax.div(me, 4)

    def device(xb, yb, cb):
        return yb * 4 + xb * 2 + cb

    xn, yn, pt = device(1 - xbit, ybit, core), device(xbit, 1 - ybit, core), device(xbit, ybit, 1 - core)
    dg = device(1 - xbit, 1 - ybit, core)
    pxn, pyn, pdg = device(1 - xbit, ybit, 1 - core), device(xbit, 1 - ybit, 1 - core), device(1 - xbit, 1 - ybit, 1 - core)

    order = [(me, j) for j in range(4)] + [(pt, j) for j in range(4)]
    order += [(xn, 0), (xn, 1), (yn, 2), (yn, 3), (pxn, 0), (pxn, 1), (pyn, 2), (pyn, 3)]
    order += [(dg, 2), (dg, 0), (pdg, 2), (pdg, 0), (xn, 2), (yn, 0), (pxn, 2), (pyn, 0)]
    order += [(dg, 3), (dg, 1), (pdg, 3), (pdg, 1), (xn, 3), (yn, 1), (pxn, 3), (pyn, 1)]

    def first(dv, j):
        return pl.multiple_of(dv * ROWS + j * TILE, TILE)

    def slot_of(c):
        return c if c < KEEP else KEEP + (c - KEEP) % RING

    def load(c):
        dv, j = order[c]
        return pltpu.make_async_copy(mat.at[:, pl.ds(first(dv, j), TILE)], abuf.at[slot_of(c)], asem.at[slot_of(c)])

    def piece(p, dv, j, h):
        return rbuf.at[p, h, pl.ds(first(dv, j), TILE), :]

    def send(p, dv, j, h, to, recv):
        return pltpu.make_async_remote_copy(
            src_ref=piece(p, dv, j, h), dst_ref=piece(p, dv, j, h), send_sem=ssem.at[p, h], recv_sem=recv,
            device_id={"row": to}, device_id_type=MESH,
        )

    def arrived(p, dv, j, h, recv):
        pltpu.make_async_copy(piece(p, dv, j, h), piece(p, dv, j, h), recv).wait()

    def send_x(p, k):
        fwd, j, h = X_SLOTS[k]
        send(p, yn if fwd else me, j, h, xn, xsem.at[p, k]).start()

    def send_y(p, k):
        fwd, j, h = Y_SLOTS[k]
        send(p, xn if fwd else me, j, h, yn, ysem.at[p, k]).start()

    def share_own(p, j, h):
        send(p, me, j, h, pt, dsem.at[p, 2 * j + h]).start()

    def take(p, k):
        fwd, j, h = X_SLOTS[k]
        src = dg if fwd else xn
        arrived(p, src, j, h, xsem.at[p, k])
        send(p, src, j, h, pt, dsem.at[p, 8 + k]).start()
        fwd, j, h = Y_SLOTS[k]
        src = dg if fwd else yn
        arrived(p, src, j, h, ysem.at[p, k])
        send(p, src, j, h, pt, dsem.at[p, 20 + k]).start()

    def take_shared(p, ks):
        for k in ks:
            fwd, j, h = X_SLOTS[k]
            arrived(p, pdg if fwd else pxn, j, h, dsem.at[p, 8 + k])
            fwd, j, h = Y_SLOTS[k]
            arrived(p, pdg if fwd else pyn, j, h, dsem.at[p, 20 + k])

    def mass_of(values, rows, h):
        weighted = values * dcol[rows, :]
        return jnp.sum(weighted.reshape(-1, 8, HALF), axis=0).sum(axis=0, keepdims=True)

    def send_mass(p):
        for dx, dy, dc in [(a, b, c) for a in range(2) for b in range(2) for c in range(2)][1:]:
            to = device(lax.rem(xbit + dx, 2), lax.rem(ybit + dy, 2), lax.rem(core + dc, 2))
            pltpu.make_async_remote_copy(
                src_ref=mbuf.at[p, me], dst_ref=mbuf.at[p, me], send_sem=msend.at[p], recv_sem=mrecv.at[p],
                device_id={"row": to}, device_id_type=MESH,
            ).start()

    def wait_a(t, cs):
        for c in cs:
            if c < KEEP:
                @pl.when(t == 0)
                def _():
                    load(c).wait()
            else:
                load(c).wait()

    def refill(t, cs):
        for c in cs:
            if c < KEEP:
                continue
            if c + RING < CHUNKS:
                load(c + RING).start()
            else:
                @pl.when(t < sweeps - 1)
                def _():
                    load(c + RING - (CHUNKS - KEEP)).start()

    def wide(p, c):
        r = pl.ds(first(*order[c]), TILE)
        return jnp.concatenate([rbuf[p, 0, r, :], rbuf[p, 1, r, :]], axis=1)

    def matmul(t, p, cs, init=False):
        wait_a(t, cs)

        @pl.loop(0, ROWS // MROWS)
        def _(i):
            rows = pl.ds(pl.multiple_of(i * MROWS, MROWS), MROWS)
            total = None if init else acc[rows, :]
            for c in cs:
                part = jnp.dot(abuf[slot_of(c), rows, :], wide(p, c), preferred_element_type=jnp.float32)
                total = part if total is None else total + part
            acc[rows, :] = total

        refill(t, cs)

    def matmul_half(p, cs, h):
        @pl.loop(0, ROWS // MROWS)
        def _(i):
            rows = pl.ds(pl.multiple_of(i * MROWS, MROWS), MROWS)
            lanes = pl.ds(h * HALF, HALF)
            total = acc[rows, lanes]
            for c in cs:
                total += jnp.dot(abuf[slot_of(c), rows, :], rbuf[p, h, pl.ds(first(*order[c]), TILE), :], preferred_element_type=jnp.float32)
            acc[rows, lanes] = total

    own_rows = pltpu.make_async_copy(start, acc, lsem.at[0])
    own_rows.start()
    own_dang = pltpu.make_async_copy(dang, draw, lsem.at[1])
    own_dang.start()
    for c in range(KEEP):
        load(c).start()
    own_tele = pltpu.make_async_copy(tele, tbuf, lsem.at[2])
    own_tele.start()
    for c in range(KEEP, KEEP + RING):
        load(c).start()

    barrier = pltpu.get_barrier_semaphore()
    for dx, dy, dc in [(a, b, c) for a in range(2) for b in range(2) for c in range(2)][1:]:
        to = device(lax.rem(xbit + dx, 2), lax.rem(ybit + dy, 2), lax.rem(core + dc, 2))
        pl.semaphore_signal(barrier, inc=1, device_id={"row": to}, device_id_type=MESH)
    own_rows.wait()
    for h in range(2):
        for j in range(4):
            rbuf[0, h, pl.ds(first(me, j), TILE), :] = acc[pl.ds(j * TILE, TILE), pl.ds(h * HALF, HALF)].astype(jnp.bfloat16)
    pl.semaphore_wait(barrier, DEV - 1)
    for k in range(4):
        send_x(0, k)
        send_y(0, k)
    for h in range(2):
        for j in range(4):
            share_own(0, j, h)
    own_dang.wait()
    for i in range(ROWS // 128):
        line = jnp.broadcast_to(draw[pl.ds(i, 1), :].astype(jnp.float32), (128, 128))
        dcol[pl.ds(i * 128, 128), :] = jnp.transpose(line)
    for h in range(2):
        total = None
        for j in range(4):
            rows = pl.ds(j * TILE, TILE)
            part = mass_of(acc[rows, pl.ds(h * HALF, HALF)], rows, h)
            total = part if total is None else total + part
        mbuf[0, me, :, pl.ds(h * HALF, HALF)] = total
    send_mass(0)
    own_tele.wait()

    @pl.loop(0, sweeps)
    def _(t):
        p = lax.rem(t, 2)
        q = 1 - p
        matmul(t, p, range(0, 4), init=True)
        take(p, 0)
        send_x(p, 4)
        send_y(p, 4)
        for j in range(4):
            for h in range(2):
                arrived(p, pt, j, h, dsem.at[p, 2 * j + h])
        matmul(t, p, range(4, 8))
        take(p, 1)
        take(p, 2)
        for k in (5, 6, 7):
            send_x(p, k)
            send_y(p, k)
        take(p, 3)
        for k in (8, 9, 10, 11):
            send_x(p, k)
            send_y(p, k)
        matmul(t, p, range(8, 12))
        take_shared(p, range(0, 4))
        matmul(t, p, range(12, 16))
        for s in range(3):
            take(p, 4 + 2 * s)
            take(p, 5 + 2 * s)
            matmul(t, p, range(16 + 4 * s, 18 + 4 * s))
            take_shared(p, (4 + 2 * s, 5 + 2 * s))
            matmul(t, p, range(18 + 4 * s, 20 + 4 * s))
        wait_a(t, range(28, 32))
        pltpu.make_async_copy(mbuf.at[p, pl.ds(0, DEV - 1)], mbuf.at[p, pl.ds(0, DEV - 1)], mrecv.at[p]).wait()
        pltpu.make_async_copy(mbuf.at[p, pl.ds(0, DEV - 1)], mbuf.at[p, pl.ds(0, DEV - 1)], msend.at[p]).wait()
        mass = jnp.sum(mbuf[p], axis=0)
        factor = damp[t]
        nodes = DEV * ROWS
        for h in range(2):
            take(p, 10 + h)
            matmul_half(p, (28, 29), h)
            take_shared(p, (10 + h,))
            sent = rbuf.at[p, h, pl.ds(0, 28 * TILE), :]
            pltpu.make_async_copy(sent, sent, ssem.at[p, h]).wait()
            lanes = pl.ds(h * HALF, HALF)
            row = (factor / nodes) * mass[:, h * HALF:(h + 1) * HALF]
            held = None
            for j in (0, 2, 1, 3):
                rows = pl.ds(j * TILE, TILE)
                total = acc[rows, lanes]
                for c in (30, 31):
                    total += jnp.dot(abuf[slot_of(c), rows, :], rbuf[p, h, pl.ds(first(*order[c]), TILE), :], preferred_element_type=jnp.float32)
                new = factor * total + (1.0 - factor) * tbuf[rows, lanes] + row
                acc[rows, lanes] = new
                rbuf[q, h, pl.ds(first(me, j), TILE), :] = new.astype(jnp.bfloat16)
                part = mass_of(new, rows, h)
                held = part if held is None else held + part

                @pl.when(t < sweeps - 1)
                def _():
                    if j in (0, 1):
                        send_x(q, j + 2 * h)
                    else:
                        send_y(q, j - 2 + 2 * h)
                    share_own(q, j, h)

                if h == 1:
                    @pl.when(t == sweeps - 1)
                    def _():
                        pltpu.make_async_copy(acc.at[rows, :], out.at[rows, :], osem.at[j]).start()
            mbuf[q, me, :, lanes] = held
        refill(t, range(28, 32))

        @pl.when(t < sweeps - 1)
        def _():
            send_mass(q)

    for j in range(4):
        rows = pl.ds(j * TILE, TILE)
        pltpu.make_async_copy(acc.at[rows, :], out.at[rows, :], osem.at[j]).wait()


def solution(mesh):
    spec_rows = P(("batch", "row"), None)
    spec_vec = P(("batch", "row"))

    def local_sweeps(mat_rows, tele_rows, dang_rows, damping, start_rows):
        sweeps = damping.shape[0]
        hbm = pl.BlockSpec(memory_space=pl.ANY)
        return pl.pallas_call(
            functools.partial(kernel, sweeps),
            out_shape=jax.ShapeDtypeStruct((ROWS, COLS), jnp.float32),
            in_specs=[hbm, hbm, hbm, pl.BlockSpec(memory_space=pltpu.SMEM), hbm],
            out_specs=hbm,
            scratch_shapes=[
                pltpu.VMEM((2, 2, DEV * ROWS, HALF), jnp.bfloat16),
                pltpu.VMEM((KEEP + RING, ROWS, TILE), jnp.bfloat16),
                pltpu.VMEM((ROWS, COLS), jnp.float32),
                pltpu.VMEM((ROWS, COLS), jnp.float32),
                pltpu.VMEM((ROWS, HALF), jnp.float32),
                pltpu.VMEM((ROWS // 128, 128), jnp.int32),
                pltpu.VMEM((2, DEV, 1, COLS), jnp.float32),
                pltpu.SemaphoreType.DMA((KEEP + RING,)),
                pltpu.SemaphoreType.DMA((3,)),
                pltpu.SemaphoreType.DMA((2, 2)),
                pltpu.SemaphoreType.DMA((2, 12)),
                pltpu.SemaphoreType.DMA((2, 12)),
                pltpu.SemaphoreType.DMA((2, 32)),
                pltpu.SemaphoreType.DMA((2,)),
                pltpu.SemaphoreType.DMA((2,)),
                pltpu.SemaphoreType.DMA((4,)),
            ],
            compiler_params=pltpu.CompilerParams(collective_id=0, has_side_effects=True, vmem_limit_bytes=67043328),
            name="sweeps",
        )(mat_rows, tele_rows, dang_rows.reshape(ROWS // 128, 128), damping, start_rows)

    return jax.shard_map(local_sweeps, mesh=mesh, in_specs=(spec_rows, spec_rows, spec_vec, P(None), spec_rows), out_specs=spec_rows, check_vma=False)
```

```python
import functools

import jax
import jax.numpy as jnp
from jax import lax
from jax.experimental import pallas as pl
from jax.experimental.pallas import tpu as pltpu
from jax.sharding import PartitionSpec as P

MESH = pl.DeviceIdType.MESH

DEV = 8
ROWS = 2048
TILE = 512
HALF = 128
COLS = 256
KEPT = (0, 1, 2, 3, 14, 15, 24, 25, 26, 27, 28, 29, 30, 31)
STREAMED = tuple(c for c in range(32) if c not in KEPT)
RING = 6
MROWS = 1024

X_SLOTS = ((0, 0, 0), (0, 1, 0), (0, 0, 1), (0, 1, 1), (1, 2, 0), (1, 2, 1), (0, 2, 0), (0, 2, 1), (1, 3, 0), (0, 3, 0), (1, 3, 1), (0, 3, 1))
Y_SLOTS = ((0, 2, 0), (0, 3, 0), (0, 2, 1), (0, 3, 1), (1, 0, 0), (1, 0, 1), (0, 0, 0), (0, 0, 1), (1, 1, 0), (0, 1, 0), (1, 1, 1), (0, 1, 1))


def kernel(sweeps, mat, tele, dang, damp, start, out, factors, rbuf, abuf, acc, tbuf, dcol, draw, mbuf, asem, lsem, ssem, xsem, ysem, dsem, msend, mrecv, osem):
    me = lax.axis_index("row")
    core = lax.rem(me, 2)
    xbit = lax.rem(lax.div(me, 2), 2)
    ybit = lax.div(me, 4)

    def device(xb, yb, cb):
        return yb * 4 + xb * 2 + cb

    xn, yn, pt = device(1 - xbit, ybit, core), device(xbit, 1 - ybit, core), device(xbit, ybit, 1 - core)
    dg = device(1 - xbit, 1 - ybit, core)
    pxn, pyn, pdg = device(1 - xbit, ybit, 1 - core), device(xbit, 1 - ybit, 1 - core), device(1 - xbit, 1 - ybit, 1 - core)

    order = [(me, j) for j in range(4)] + [(pt, j) for j in range(4)]
    order += [(xn, 0), (xn, 1), (yn, 2), (yn, 3), (pxn, 0), (pxn, 1), (pyn, 2), (pyn, 3)]
    order += [(dg, 2), (dg, 0), (pdg, 2), (pdg, 0), (xn, 2), (yn, 0), (pxn, 2), (pyn, 0)]
    order += [(dg, 3), (dg, 1), (pdg, 3), (pdg, 1), (xn, 3), (yn, 1), (pxn, 3), (pyn, 1)]

    def first(dv, j):
        return pl.multiple_of(dv * ROWS + j * TILE, TILE)

    def slot_of(c):
        return KEPT.index(c) if c in KEPT else len(KEPT) + STREAMED.index(c) % RING

    def load(c):
        dv, j = order[c]
        return pltpu.make_async_copy(mat.at[:, pl.ds(first(dv, j), TILE)], abuf.at[slot_of(c)], asem.at[slot_of(c)])

    def piece(p, dv, j, h):
        return rbuf.at[p, h, pl.ds(first(dv, j), TILE), :]

    def send(p, dv, j, h, to, recv):
        return pltpu.make_async_remote_copy(
            src_ref=piece(p, dv, j, h), dst_ref=piece(p, dv, j, h), send_sem=ssem.at[p, h], recv_sem=recv,
            device_id={"row": to}, device_id_type=MESH,
        )

    def arrived(p, dv, j, h, recv):
        pltpu.make_async_copy(piece(p, dv, j, h), piece(p, dv, j, h), recv).wait()

    def send_x(p, k):
        fwd, j, h = X_SLOTS[k]
        send(p, yn if fwd else me, j, h, xn, xsem.at[p, k]).start()

    def send_y(p, k):
        fwd, j, h = Y_SLOTS[k]
        send(p, xn if fwd else me, j, h, yn, ysem.at[p, k]).start()

    def share_own(p, j, h):
        send(p, me, j, h, pt, dsem.at[p, 2 * j + h]).start()

    def take(p, k):
        fwd, j, h = X_SLOTS[k]
        src = dg if fwd else xn
        arrived(p, src, j, h, xsem.at[p, k])
        send(p, src, j, h, pt, dsem.at[p, 8 + k]).start()
        fwd, j, h = Y_SLOTS[k]
        src = dg if fwd else yn
        arrived(p, src, j, h, ysem.at[p, k])
        send(p, src, j, h, pt, dsem.at[p, 20 + k]).start()

    def take_shared(p, ks):
        for k in ks:
            fwd, j, h = X_SLOTS[k]
            arrived(p, pdg if fwd else pxn, j, h, dsem.at[p, 8 + k])
            fwd, j, h = Y_SLOTS[k]
            arrived(p, pdg if fwd else pyn, j, h, dsem.at[p, 20 + k])

    def mass_of(values, rows, h):
        weighted = values * dcol[rows, :]
        return jnp.sum(weighted.reshape(-1, 8, HALF), axis=0).sum(axis=0, keepdims=True)

    def send_mass(p):
        for dx, dy, dc in [(a, b, c) for a in range(2) for b in range(2) for c in range(2)][1:]:
            to = device(lax.rem(xbit + dx, 2), lax.rem(ybit + dy, 2), lax.rem(core + dc, 2))
            pltpu.make_async_remote_copy(
                src_ref=mbuf.at[p, me], dst_ref=mbuf.at[p, me], send_sem=msend.at[p], recv_sem=mrecv.at[p],
                device_id={"row": to}, device_id_type=MESH,
            ).start()

    def wait_a(t, cs):
        for c in cs:
            if c in KEPT:
                @pl.when(t == 0)
                def _():
                    load(c).wait()
            else:
                load(c).wait()

    def refill(t, cs):
        for c in cs:
            if c in KEPT:
                continue
            later = STREAMED.index(c) + RING
            if later < len(STREAMED):
                load(STREAMED[later]).start()
            else:
                @pl.when(t < sweeps - 1)
                def _():
                    load(STREAMED[later - len(STREAMED)]).start()

    def wide(p, c):
        r = pl.ds(first(*order[c]), TILE)
        return jnp.concatenate([rbuf[p, 0, r, :], rbuf[p, 1, r, :]], axis=1)

    def matmul(t, p, cs, init=False):
        wait_a(t, cs)

        @pl.loop(0, ROWS // MROWS)
        def _(i):
            rows = pl.ds(pl.multiple_of(i * MROWS, MROWS), MROWS)
            total = None if init else acc[rows, :]
            for c in cs:
                part = jnp.dot(abuf[slot_of(c), rows, :], wide(p, c), preferred_element_type=jnp.float32)
                total = part if total is None else total + part
            acc[rows, :] = total

        refill(t, cs)

    def matmul_half(p, cs, h):
        @pl.loop(0, ROWS // MROWS)
        def _(i):
            rows = pl.ds(pl.multiple_of(i * MROWS, MROWS), MROWS)
            lanes = pl.ds(h * HALF, HALF)
            total = acc[rows, lanes]
            for c in cs:
                total += jnp.dot(abuf[slot_of(c), rows, :], rbuf[p, h, pl.ds(first(*order[c]), TILE), :], preferred_element_type=jnp.float32)
            acc[rows, lanes] = total

    own_rows = pltpu.make_async_copy(start, acc, lsem.at[0])
    own_rows.start()
    own_dang = pltpu.make_async_copy(dang, draw, lsem.at[1])
    own_dang.start()
    own_damp = pltpu.make_async_copy(damp, factors, lsem.at[3])
    own_damp.start()
    for c in sorted(KEPT + STREAMED[:RING]):
        load(c).start()
    own_tele = pltpu.make_async_copy(tele, tbuf, lsem.at[2])
    own_tele.start()

    barrier = pltpu.get_barrier_semaphore()
    for dx, dy, dc in [(a, b, c) for a in range(2) for b in range(2) for c in range(2)][1:]:
        to = device(lax.rem(xbit + dx, 2), lax.rem(ybit + dy, 2), lax.rem(core + dc, 2))
        pl.semaphore_signal(barrier, inc=1, device_id={"row": to}, device_id_type=MESH)
    own_rows.wait()
    for h in range(2):
        for j in range(4):
            rbuf[0, h, pl.ds(first(me, j), TILE), :] = acc[pl.ds(j * TILE, TILE), pl.ds(h * HALF, HALF)].astype(jnp.bfloat16)
    pl.semaphore_wait(barrier, DEV - 1)
    for k in range(4):
        send_x(0, k)
        send_y(0, k)
    for h in range(2):
        for j in range(4):
            share_own(0, j, h)
    own_dang.wait()
    for i in range(ROWS // 128):
        line = jnp.broadcast_to(draw[pl.ds(i, 1), :].astype(jnp.float32), (128, 128))
        dcol[pl.ds(i * 128, 128), :] = jnp.transpose(line)
    for h in range(2):
        total = None
        for j in range(4):
            rows = pl.ds(j * TILE, TILE)
            part = mass_of(acc[rows, pl.ds(h * HALF, HALF)], rows, h)
            total = part if total is None else total + part
        mbuf[0, me, :, pl.ds(h * HALF, HALF)] = total
    send_mass(0)
    own_tele.wait()
    own_damp.wait()

    @pl.loop(0, sweeps)
    def _(t):
        p = lax.rem(t, 2)
        q = 1 - p
        matmul(t, p, range(0, 4), init=True)
        take(p, 0)
        send_x(p, 4)
        send_y(p, 4)
        for j in range(4):
            for h in range(2):
                arrived(p, pt, j, h, dsem.at[p, 2 * j + h])
        matmul(t, p, range(4, 8))
        take(p, 1)
        take(p, 2)
        for k in (5, 6, 7):
            send_x(p, k)
            send_y(p, k)
        take(p, 3)
        for k in (8, 9, 10, 11):
            send_x(p, k)
            send_y(p, k)
        matmul(t, p, range(8, 12))
        take_shared(p, range(0, 4))
        matmul(t, p, range(12, 16))
        for s in range(2):
            take(p, 4 + 2 * s)
            take(p, 5 + 2 * s)
            matmul(t, p, range(16 + 4 * s, 18 + 4 * s))
            take_shared(p, (4 + 2 * s, 5 + 2 * s))
            matmul(t, p, range(18 + 4 * s, 20 + 4 * s))
        wait_a(t, range(24, 32))
        pltpu.make_async_copy(mbuf.at[p, pl.ds(0, DEV - 1)], mbuf.at[p, pl.ds(0, DEV - 1)], mrecv.at[p]).wait()
        pltpu.make_async_copy(mbuf.at[p, pl.ds(0, DEV - 1)], mbuf.at[p, pl.ds(0, DEV - 1)], msend.at[p]).wait()
        mass = jnp.sum(mbuf[p], axis=0)
        factor = factors[t]
        nodes = DEV * ROWS
        for h in range(2):
            take(p, 8 + 2 * h)
            matmul_half(p, (24, 25), h)
            take_shared(p, (8 + 2 * h,))
            matmul_half(p, (26, 27), h)
            take(p, 9 + 2 * h)
            matmul_half(p, (28, 29), h)
            take_shared(p, (9 + 2 * h,))
            sent = rbuf.at[p, h, pl.ds(0, 28 * TILE), :]
            pltpu.make_async_copy(sent, sent, ssem.at[p, h]).wait()
            lanes = pl.ds(h * HALF, HALF)
            row = (factor / nodes) * mass[:, h * HALF:(h + 1) * HALF]
            held = None
            for j in (0, 2, 1, 3):
                rows = pl.ds(j * TILE, TILE)
                total = acc[rows, lanes]
                for c in (30, 31):
                    total += jnp.dot(abuf[slot_of(c), rows, :], rbuf[p, h, pl.ds(first(*order[c]), TILE), :], preferred_element_type=jnp.float32)
                new = factor * total + (1.0 - factor) * tbuf[rows, lanes] + row
                acc[rows, lanes] = new
                rbuf[q, h, pl.ds(first(me, j), TILE), :] = new.astype(jnp.bfloat16)
                part = mass_of(new, rows, h)
                held = part if held is None else held + part

                @pl.when(t < sweeps - 1)
                def _():
                    if j in (0, 1):
                        send_x(q, j + 2 * h)
                    else:
                        send_y(q, j - 2 + 2 * h)
                    share_own(q, j, h)

                @pl.when(t == sweeps - 1)
                def _():
                    pltpu.make_async_copy(acc.at[rows, lanes], out.at[rows, lanes], osem.at[h, j]).start()
            mbuf[q, me, :, lanes] = held

        @pl.when(t < sweeps - 1)
        def _():
            send_mass(q)

    for h in range(2):
        for j in range(4):
            part = (pl.ds(j * TILE, TILE), pl.ds(h * HALF, HALF))
            pltpu.make_async_copy(acc.at[part], out.at[part], osem.at[h, j]).wait()


def solution(mesh):
    spec_rows = P(("batch", "row"), None)
    spec_vec = P(("batch", "row"))

    def local_sweeps(mat_rows, tele_rows, dang_rows, damping, start_rows):
        sweeps = damping.shape[0]
        hbm = pl.BlockSpec(memory_space=pl.ANY)
        return pl.pallas_call(
            functools.partial(kernel, sweeps),
            out_shape=jax.ShapeDtypeStruct((ROWS, COLS), jnp.float32),
            in_specs=[hbm] * 5,
            out_specs=hbm,
            scratch_shapes=[
                pltpu.SMEM((sweeps,), jnp.float32),
                pltpu.VMEM((2, 2, DEV * ROWS, HALF), jnp.bfloat16),
                pltpu.VMEM((len(KEPT) + RING, ROWS, TILE), jnp.bfloat16),
                pltpu.VMEM((ROWS, COLS), jnp.float32),
                pltpu.VMEM((ROWS, COLS), jnp.float32),
                pltpu.VMEM((ROWS, HALF), jnp.float32),
                pltpu.VMEM((ROWS // 128, 128), jnp.int32),
                pltpu.VMEM((2, DEV, 1, COLS), jnp.float32),
                pltpu.SemaphoreType.DMA((len(KEPT) + RING,)),
                pltpu.SemaphoreType.DMA((4,)),
                pltpu.SemaphoreType.DMA((2, 2)),
                pltpu.SemaphoreType.DMA((2, 12)),
                pltpu.SemaphoreType.DMA((2, 12)),
                pltpu.SemaphoreType.DMA((2, 32)),
                pltpu.SemaphoreType.DMA((2,)),
                pltpu.SemaphoreType.DMA((2,)),
                pltpu.SemaphoreType.DMA((2, 4)),
            ],
            compiler_params=pltpu.CompilerParams(collective_id=0, has_side_effects=True, vmem_limit_bytes=67043328),
            name="sweeps",
        )(mat_rows, tele_rows, dang_rows.reshape(ROWS // 128, 128), damping, start_rows)

    return jax.shard_map(local_sweeps, mesh=mesh, in_specs=(spec_rows, spec_rows, spec_vec, P(None), spec_rows), out_specs=spec_rows, check_vma=False)
```

```python
import functools

import jax
import jax.numpy as jnp
from jax import lax
from jax.experimental import pallas as pl
from jax.experimental.pallas import tpu as pltpu
from jax.sharding import PartitionSpec as P

MESH = pl.DeviceIdType.MESH

DEV = 8
ROWS = 2048
TILE = 512
HALF = 128
COLS = 256
KEPT = (0, 1, 2, 3, 14, 15, 24, 25, 26, 27, 28, 29, 30, 31)
STREAMED = tuple(c for c in range(32) if c not in KEPT)
RING = 6
MROWS = 1024

X_SLOTS = ((0, 0, 0), (0, 2, 0), (0, 0, 1), (0, 2, 1), (0, 1, 0), (0, 1, 1), (1, 1, 0), (1, 1, 1), (1, 3, 0), (0, 3, 0), (1, 3, 1), (0, 3, 1))
Y_SLOTS = ((0, 1, 0), (0, 3, 0), (0, 1, 1), (0, 3, 1), (0, 0, 0), (0, 0, 1), (1, 0, 0), (1, 0, 1), (1, 2, 0), (0, 2, 0), (1, 2, 1), (0, 2, 1))


def kernel(sweeps, mat, tele, dang, damp, start, out, factors, rbuf, abuf, acc, tbuf, dcol, draw, mbuf, asem, lsem, ssem, xsem, ysem, dsem, msend, mrecv, osem):
    me = lax.axis_index("row")
    core = lax.rem(me, 2)
    xbit = lax.rem(lax.div(me, 2), 2)
    ybit = lax.div(me, 4)

    def device(xb, yb, cb):
        return yb * 4 + xb * 2 + cb

    xn, yn, pt = device(1 - xbit, ybit, core), device(xbit, 1 - ybit, core), device(xbit, ybit, 1 - core)
    dg = device(1 - xbit, 1 - ybit, core)
    pxn, pyn, pdg = device(1 - xbit, ybit, 1 - core), device(xbit, 1 - ybit, 1 - core), device(1 - xbit, 1 - ybit, 1 - core)

    order = [(me, j) for j in range(4)] + [(pt, j) for j in range(4)]
    order += [(xn, 0), (xn, 2), (yn, 1), (yn, 3), (pxn, 0), (pxn, 2), (pyn, 1), (pyn, 3)]
    order += [(xn, 1), (yn, 0), (pxn, 1), (pyn, 0), (dg, 1), (dg, 0), (pdg, 1), (pdg, 0)]
    order += [(dg, 3), (dg, 2), (pdg, 3), (pdg, 2), (xn, 3), (yn, 2), (pxn, 3), (pyn, 2)]

    def first(dv, j):
        return pl.multiple_of(dv * ROWS + j * TILE, TILE)

    def slot_of(c):
        return KEPT.index(c) if c in KEPT else len(KEPT) + STREAMED.index(c) % RING

    def load(c):
        dv, j = order[c]
        return pltpu.make_async_copy(mat.at[:, pl.ds(first(dv, j), TILE)], abuf.at[slot_of(c)], asem.at[slot_of(c)])

    def piece(p, dv, j, h):
        return rbuf.at[p, h, pl.ds(first(dv, j), TILE), :]

    def send(p, dv, j, h, to, recv):
        return pltpu.make_async_remote_copy(
            src_ref=piece(p, dv, j, h), dst_ref=piece(p, dv, j, h), send_sem=ssem.at[p, h], recv_sem=recv,
            device_id={"row": to}, device_id_type=MESH,
        )

    def arrived(p, dv, j, h, recv):
        pltpu.make_async_copy(piece(p, dv, j, h), piece(p, dv, j, h), recv).wait()

    def send_x(p, k):
        fwd, j, h = X_SLOTS[k]
        send(p, yn if fwd else me, j, h, xn, xsem.at[p, k]).start()

    def send_y(p, k):
        fwd, j, h = Y_SLOTS[k]
        send(p, xn if fwd else me, j, h, yn, ysem.at[p, k]).start()

    def share_own(p, j, h):
        send(p, me, j, h, pt, dsem.at[p, 2 * j + h]).start()

    def take(p, k):
        fwd, j, h = X_SLOTS[k]
        src = dg if fwd else xn
        arrived(p, src, j, h, xsem.at[p, k])
        send(p, src, j, h, pt, dsem.at[p, 8 + k]).start()
        fwd, j, h = Y_SLOTS[k]
        src = dg if fwd else yn
        arrived(p, src, j, h, ysem.at[p, k])
        send(p, src, j, h, pt, dsem.at[p, 20 + k]).start()

    def take_shared(p, ks):
        for k in ks:
            fwd, j, h = X_SLOTS[k]
            arrived(p, pdg if fwd else pxn, j, h, dsem.at[p, 8 + k])
            fwd, j, h = Y_SLOTS[k]
            arrived(p, pdg if fwd else pyn, j, h, dsem.at[p, 20 + k])

    def mass_of(values, rows, h):
        weighted = values * dcol[rows, :]
        return jnp.sum(weighted.reshape(-1, 8, HALF), axis=0).sum(axis=0, keepdims=True)

    def send_mass(p):
        for dx, dy, dc in [(a, b, c) for a in range(2) for b in range(2) for c in range(2)][1:]:
            to = device(lax.rem(xbit + dx, 2), lax.rem(ybit + dy, 2), lax.rem(core + dc, 2))
            pltpu.make_async_remote_copy(
                src_ref=mbuf.at[p, me], dst_ref=mbuf.at[p, me], send_sem=msend.at[p], recv_sem=mrecv.at[p],
                device_id={"row": to}, device_id_type=MESH,
            ).start()

    def wait_a(t, cs):
        for c in cs:
            if c in KEPT:
                @pl.when(t == 0)
                def _():
                    load(c).wait()
            else:
                load(c).wait()

    def refill(t, cs):
        for c in cs:
            if c in KEPT:
                continue
            later = STREAMED.index(c) + RING
            if later < len(STREAMED):
                load(STREAMED[later]).start()
            else:
                @pl.when(t < sweeps - 1)
                def _():
                    load(STREAMED[later - len(STREAMED)]).start()

    def wide(p, c):
        r = pl.ds(first(*order[c]), TILE)
        return jnp.concatenate([rbuf[p, 0, r, :], rbuf[p, 1, r, :]], axis=1)

    def matmul(t, p, cs, init=False):
        wait_a(t, cs)

        for i in range(ROWS // MROWS):
            rows = pl.ds(i * MROWS, MROWS)
            total = None if init else acc[rows, :]
            for c in cs:
                part = jnp.dot(abuf[slot_of(c), rows, :], wide(p, c), preferred_element_type=jnp.float32)
                total = part if total is None else total + part
            acc[rows, :] = total

        refill(t, cs)

    def matmul_half(p, cs, h):
        for i in range(ROWS // MROWS):
            rows = pl.ds(i * MROWS, MROWS)
            lanes = pl.ds(h * HALF, HALF)
            total = acc[rows, lanes]
            for c in cs:
                total += jnp.dot(abuf[slot_of(c), rows, :], rbuf[p, h, pl.ds(first(*order[c]), TILE), :], preferred_element_type=jnp.float32)
            acc[rows, lanes] = total

    barrier = pltpu.get_barrier_semaphore()
    for dx, dy, dc in [(a, b, c) for a in range(2) for b in range(2) for c in range(2)][1:]:
        to = device(lax.rem(xbit + dx, 2), lax.rem(ybit + dy, 2), lax.rem(core + dc, 2))
        pl.semaphore_signal(barrier, inc=1, device_id={"row": to}, device_id_type=MESH)
    own_rows = []
    for j in range(4):
        rows = pl.ds(j * TILE, TILE)
        own_rows.append(pltpu.make_async_copy(start.at[rows, :], acc.at[rows, :], lsem.at[3 + j]))
        own_rows[j].start()
    own_dang = pltpu.make_async_copy(dang, draw, lsem.at[0])
    own_dang.start()
    own_damp = pltpu.make_async_copy(damp, factors, lsem.at[1])
    own_damp.start()
    for c in sorted(KEPT + STREAMED[:RING]):
        load(c).start()
    own_tele = pltpu.make_async_copy(tele, tbuf, lsem.at[2])
    own_tele.start()
    for j in range(4):
        own_rows[j].wait()
        for h in range(2):
            rbuf[0, h, pl.ds(first(me, j), TILE), :] = acc[pl.ds(j * TILE, TILE), pl.ds(h * HALF, HALF)].astype(jnp.bfloat16)
        if j == 1:
            pl.semaphore_wait(barrier, DEV - 1)
            send_x(0, 0)
            send_y(0, 0)
    for k in range(1, 6):
        send_x(0, k)
        send_y(0, k)
    for h in range(2):
        for j in range(4):
            share_own(0, j, h)
    own_dang.wait()
    for i in range(ROWS // 128):
        line = jnp.broadcast_to(draw[pl.ds(i, 1), :].astype(jnp.float32), (128, 128))
        dcol[pl.ds(i * 128, 128), :] = jnp.transpose(line)
    for h in range(2):
        total = None
        for j in range(4):
            rows = pl.ds(j * TILE, TILE)
            part = mass_of(acc[rows, pl.ds(h * HALF, HALF)], rows, h)
            total = part if total is None else total + part
        mbuf[0, me, :, pl.ds(h * HALF, HALF)] = total
    send_mass(0)
    own_tele.wait()
    own_damp.wait()

    @pl.loop(0, sweeps)
    def _(t):
        p = lax.rem(t, 2)
        q = 1 - p
        for j in range(4):
            for h in range(2):
                arrived(p, pt, j, h, dsem.at[p, 2 * j + h])
        matmul(t, p, range(0, 8), init=True)
        for k in range(3):
            take(p, k)
        for k in (6, 7, 8, 9):
            send_x(p, k)
            send_y(p, k)
        take(p, 3)
        for k in (10, 11):
            send_x(p, k)
            send_y(p, k)
        matmul(t, p, range(8, 12))
        take_shared(p, range(0, 4))
        matmul(t, p, range(12, 16))
        for s in range(2):
            take(p, 4 + 2 * s)
            take(p, 5 + 2 * s)
            matmul(t, p, range(16 + 4 * s, 18 + 4 * s))
            take_shared(p, (4 + 2 * s, 5 + 2 * s))
            matmul(t, p, range(18 + 4 * s, 20 + 4 * s))
        wait_a(t, range(24, 32))
        pltpu.make_async_copy(mbuf.at[p, pl.ds(0, DEV - 1)], mbuf.at[p, pl.ds(0, DEV - 1)], mrecv.at[p]).wait()
        pltpu.make_async_copy(mbuf.at[p, pl.ds(0, DEV - 1)], mbuf.at[p, pl.ds(0, DEV - 1)], msend.at[p]).wait()
        mass = jnp.sum(mbuf[p], axis=0)
        factor = factors[t]
        nodes = DEV * ROWS
        for h in range(2):
            take(p, 8 + 2 * h)
            matmul_half(p, (24, 25), h)
            take_shared(p, (8 + 2 * h,))
            matmul_half(p, (26, 27), h)
            take(p, 9 + 2 * h)
            matmul_half(p, (28, 29), h)
            take_shared(p, (9 + 2 * h,))
            sent = rbuf.at[p, h, pl.ds(0, 28 * TILE), :]
            pltpu.make_async_copy(sent, sent, ssem.at[p, h]).wait()
            lanes = pl.ds(h * HALF, HALF)
            row = (factor / nodes) * mass[:, h * HALF:(h + 1) * HALF]
            held = None
            for i in range(ROWS // MROWS):
                rows = pl.ds(i * MROWS, MROWS)
                total = acc[rows, lanes]
                for c in (30, 31):
                    total += jnp.dot(abuf[slot_of(c), rows, :], rbuf[p, h, pl.ds(first(*order[c]), TILE), :], preferred_element_type=jnp.float32)
                new = factor * total + (1.0 - factor) * tbuf[rows, lanes] + row
                acc[rows, lanes] = new
                rbuf[q, h, pl.ds(first(me, 2 * i), MROWS), :] = new.astype(jnp.bfloat16)
                part = mass_of(new, rows, h)
                held = part if held is None else held + part

                @pl.when(t < sweeps - 1)
                def _():
                    send_x(q, i + 2 * h)
                    send_y(q, i + 2 * h)
                    share_own(q, 2 * i, h)
                    share_own(q, 2 * i + 1, h)
                    if i + h == 2:
                        for k in (4, 5):
                            send_x(q, k)
                            send_y(q, k)

                @pl.when(t == sweeps - 1)
                def _():
                    pltpu.make_async_copy(acc.at[rows, lanes], out.at[rows, lanes], osem.at[h, i]).start()

            mbuf[q, me, :, lanes] = held

        @pl.when(t < sweeps - 1)
        def _():
            send_mass(q)

    for h in range(2):
        for i in range(ROWS // MROWS):
            part = (pl.ds(i * MROWS, MROWS), pl.ds(h * HALF, HALF))
            pltpu.make_async_copy(acc.at[part], out.at[part], osem.at[h, i]).wait()


def solution(mesh):
    spec_rows = P(("batch", "row"), None)
    spec_vec = P(("batch", "row"))

    def local_sweeps(mat_rows, tele_rows, dang_rows, damping, start_rows):
        sweeps = damping.shape[0]
        hbm = pl.BlockSpec(memory_space=pl.ANY)
        return pl.pallas_call(
            functools.partial(kernel, sweeps),
            out_shape=jax.ShapeDtypeStruct((ROWS, COLS), jnp.float32),
            in_specs=[hbm] * 5,
            out_specs=hbm,
            scratch_shapes=[
                pltpu.SMEM((sweeps,), jnp.float32),
                pltpu.VMEM((2, 2, DEV * ROWS, HALF), jnp.bfloat16),
                pltpu.VMEM((len(KEPT) + RING, ROWS, TILE), jnp.bfloat16),
                pltpu.VMEM((ROWS, COLS), jnp.float32),
                pltpu.VMEM((ROWS, COLS), jnp.float32),
                pltpu.VMEM((ROWS, HALF), jnp.float32),
                pltpu.VMEM((ROWS // 128, 128), jnp.int32),
                pltpu.VMEM((2, DEV, 1, COLS), jnp.float32),
                pltpu.SemaphoreType.DMA((len(KEPT) + RING,)),
                pltpu.SemaphoreType.DMA((7,)),
                pltpu.SemaphoreType.DMA((2, 2)),
                pltpu.SemaphoreType.DMA((2, 12)),
                pltpu.SemaphoreType.DMA((2, 12)),
                pltpu.SemaphoreType.DMA((2, 32)),
                pltpu.SemaphoreType.DMA((2,)),
                pltpu.SemaphoreType.DMA((2,)),
                pltpu.SemaphoreType.DMA((2, 2)),
            ],
            compiler_params=pltpu.CompilerParams(collective_id=0, has_side_effects=True, vmem_limit_bytes=67043328),
            name="sweeps",
        )(mat_rows, tele_rows, dang_rows.reshape(ROWS // 128, 128), damping, start_rows)

    return jax.shard_map(local_sweeps, mesh=mesh, in_specs=(spec_rows, spec_rows, spec_vec, P(None), spec_rows), out_specs=spec_rows, check_vma=False)
```

```python
import functools

import jax
import jax.numpy as jnp
from jax import lax
from jax.experimental import pallas as pl
from jax.experimental.pallas import tpu as pltpu
from jax.sharding import PartitionSpec as P

MESH = pl.DeviceIdType.MESH

DEV = 8
ROWS = 2048
TILE = 512
HALF = 128
COLS = 256
KEPT = (0, 1, 2, 3, 14, 15, 24, 25, 26, 27, 28, 29, 30, 31)
STREAMED = tuple(c for c in range(32) if c not in KEPT)
RING = 6
MROWS = 512
SENT = 1024

X_SLOTS = ((0, 0, 0), (0, 2, 0), (0, 0, 1), (0, 2, 1), (0, 1, 0), (0, 1, 1), (1, 1, 0), (1, 1, 1), (1, 3, 0), (0, 3, 0), (1, 3, 1), (0, 3, 1))
Y_SLOTS = ((0, 1, 0), (0, 3, 0), (0, 1, 1), (0, 3, 1), (0, 0, 0), (0, 0, 1), (1, 0, 0), (1, 0, 1), (1, 2, 0), (0, 2, 0), (1, 2, 1), (0, 2, 1))


def kernel(sweeps, mat, tele, dang, damp, start, acc, factors, rbuf, abuf, tbuf, dcol, draw, mbuf, asem, lsem, ssem, xsem, ysem, dsem, msend, mrecv):
    me = lax.axis_index("row")
    core = lax.rem(me, 2)
    xbit = lax.rem(lax.div(me, 2), 2)
    ybit = lax.div(me, 4)

    def device(xb, yb, cb):
        return yb * 4 + xb * 2 + cb

    xn, yn, pt = device(1 - xbit, ybit, core), device(xbit, 1 - ybit, core), device(xbit, ybit, 1 - core)
    dg = device(1 - xbit, 1 - ybit, core)
    pxn, pyn, pdg = device(1 - xbit, ybit, 1 - core), device(xbit, 1 - ybit, 1 - core), device(1 - xbit, 1 - ybit, 1 - core)

    order = [(me, j) for j in range(4)] + [(pt, j) for j in range(4)]
    order += [(xn, 0), (xn, 2), (yn, 1), (yn, 3), (pxn, 0), (pxn, 2), (pyn, 1), (pyn, 3)]
    order += [(xn, 1), (yn, 0), (pxn, 1), (pyn, 0), (dg, 1), (dg, 0), (pdg, 1), (pdg, 0)]
    order += [(dg, 3), (dg, 2), (pdg, 3), (pdg, 2), (xn, 3), (yn, 2), (pxn, 3), (pyn, 2)]

    def first(dv, j):
        return pl.multiple_of(dv * ROWS + j * TILE, TILE)

    def slot_of(c):
        return KEPT.index(c) if c in KEPT else len(KEPT) + STREAMED.index(c) % RING

    def load(c):
        dv, j = order[c]
        return pltpu.make_async_copy(mat.at[:, pl.ds(first(dv, j), TILE)], abuf.at[slot_of(c)], asem.at[slot_of(c)])

    def piece(p, dv, j, h):
        return rbuf.at[p, h, pl.ds(first(dv, j), TILE), :]

    def send(p, dv, j, h, to, recv):
        return pltpu.make_async_remote_copy(
            src_ref=piece(p, dv, j, h), dst_ref=piece(p, dv, j, h), send_sem=ssem.at[p, h], recv_sem=recv,
            device_id={"row": to}, device_id_type=MESH,
        )

    def arrived(p, dv, j, h, recv):
        pltpu.make_async_copy(piece(p, dv, j, h), piece(p, dv, j, h), recv).wait()

    def send_x(p, k):
        fwd, j, h = X_SLOTS[k]
        send(p, yn if fwd else me, j, h, xn, xsem.at[p, k]).start()

    def send_y(p, k):
        fwd, j, h = Y_SLOTS[k]
        send(p, xn if fwd else me, j, h, yn, ysem.at[p, k]).start()

    def share_own(p, j, h):
        send(p, me, j, h, pt, dsem.at[p, 2 * j + h]).start()

    def take(p, k):
        fwd, j, h = X_SLOTS[k]
        src = dg if fwd else xn
        arrived(p, src, j, h, xsem.at[p, k])
        send(p, src, j, h, pt, dsem.at[p, 8 + k]).start()
        fwd, j, h = Y_SLOTS[k]
        src = dg if fwd else yn
        arrived(p, src, j, h, ysem.at[p, k])
        send(p, src, j, h, pt, dsem.at[p, 20 + k]).start()

    def take_shared(p, ks):
        for k in ks:
            fwd, j, h = X_SLOTS[k]
            arrived(p, pdg if fwd else pxn, j, h, dsem.at[p, 8 + k])
            fwd, j, h = Y_SLOTS[k]
            arrived(p, pdg if fwd else pyn, j, h, dsem.at[p, 20 + k])

    def mass_of(values, rows, h):
        weighted = values * dcol[rows, :].astype(jnp.float32)
        return jnp.sum(weighted.reshape(-1, 8, HALF), axis=0).sum(axis=0, keepdims=True)

    def send_mass(p):
        for dx, dy, dc in [(a, b, c) for a in range(2) for b in range(2) for c in range(2)][1:]:
            to = device(lax.rem(xbit + dx, 2), lax.rem(ybit + dy, 2), lax.rem(core + dc, 2))
            pltpu.make_async_remote_copy(
                src_ref=mbuf.at[p, me], dst_ref=mbuf.at[p, me], send_sem=msend.at[p], recv_sem=mrecv.at[p],
                device_id={"row": to}, device_id_type=MESH,
            ).start()

    def wait_a(t, cs):
        for c in cs:
            if c in KEPT:
                @pl.when(t == 0)
                def _():
                    load(c).wait()
            else:
                load(c).wait()

    def refill(t, cs):
        for c in cs:
            if c in KEPT:
                continue
            later = STREAMED.index(c) + RING
            if later < len(STREAMED):
                load(STREAMED[later]).start()
            else:
                @pl.when(t < sweeps - 1)
                def _():
                    load(STREAMED[later - len(STREAMED)]).start()

    def wide(p, c):
        r = pl.ds(first(*order[c]), TILE)
        return jnp.concatenate([rbuf[p, 0, r, :], rbuf[p, 1, r, :]], axis=1)

    def matmul(t, p, cs, init=False):
        wait_a(t, cs)

        for i in range(ROWS // MROWS):
            rows = pl.ds(i * MROWS, MROWS)
            total = None if init else acc[rows, :]
            for c in cs:
                part = jnp.dot(abuf[slot_of(c), rows, :], wide(p, c), preferred_element_type=jnp.float32)
                total = part if total is None else total + part
            acc[rows, :] = total

        refill(t, cs)

    def matmul_half(p, cs, h):
        for i in range(ROWS // MROWS):
            rows = pl.ds(i * MROWS, MROWS)
            lanes = pl.ds(h * HALF, HALF)
            total = acc[rows, lanes]
            for c in cs:
                total += jnp.dot(abuf[slot_of(c), rows, :], rbuf[p, h, pl.ds(first(*order[c]), TILE), :], preferred_element_type=jnp.float32)
            acc[rows, lanes] = total

    barrier = pltpu.get_barrier_semaphore()
    for dx, dy, dc in [(a, b, c) for a in range(2) for b in range(2) for c in range(2)][1:]:
        to = device(lax.rem(xbit + dx, 2), lax.rem(ybit + dy, 2), lax.rem(core + dc, 2))
        pl.semaphore_signal(barrier, inc=1, device_id={"row": to}, device_id_type=MESH)
    own_rows = []
    for j in range(4):
        rows = pl.ds(j * TILE, TILE)
        own_rows.append(pltpu.make_async_copy(start.at[rows, :], acc.at[rows, :], lsem.at[3 + j]))
        own_rows[j].start()
    own_dang = pltpu.make_async_copy(dang, draw, lsem.at[0])
    own_dang.start()
    own_damp = pltpu.make_async_copy(damp, factors, lsem.at[1])
    own_damp.start()
    for c in sorted(KEPT + STREAMED[:RING]):
        load(c).start()
    own_tele = pltpu.make_async_copy(tele, tbuf, lsem.at[2])
    own_tele.start()
    for j in range(4):
        own_rows[j].wait()
        for h in range(2):
            rbuf[0, h, pl.ds(first(me, j), TILE), :] = acc[pl.ds(j * TILE, TILE), pl.ds(h * HALF, HALF)].astype(jnp.bfloat16)
        if j == 1:
            pl.semaphore_wait(barrier, DEV - 1)
            send_x(0, 0)
            send_y(0, 0)
    for k in range(1, 6):
        send_x(0, k)
        send_y(0, k)
    for h in range(2):
        for j in range(4):
            share_own(0, j, h)
    own_dang.wait()
    for i in range(ROWS // 128):
        line = jnp.broadcast_to(draw[pl.ds(i, 1), :].astype(jnp.float32), (128, 128))
        dcol[pl.ds(i * 128, 128), :] = jnp.transpose(line).astype(jnp.bfloat16)
    for h in range(2):
        total = None
        for j in range(4):
            rows = pl.ds(j * TILE, TILE)
            part = mass_of(acc[rows, pl.ds(h * HALF, HALF)], rows, h)
            total = part if total is None else total + part
        mbuf[0, me, :, pl.ds(h * HALF, HALF)] = total
    send_mass(0)
    own_tele.wait()
    own_damp.wait()

    @pl.loop(0, sweeps)
    def _(t):
        p = lax.rem(t, 2)
        q = 1 - p
        for j in range(4):
            for h in range(2):
                arrived(p, pt, j, h, dsem.at[p, 2 * j + h])
        matmul(t, p, range(0, 8), init=True)
        for k in range(3):
            take(p, k)
        for k in (6, 7, 8, 9):
            send_x(p, k)
            send_y(p, k)
        take(p, 3)
        for k in (10, 11):
            send_x(p, k)
            send_y(p, k)
        matmul(t, p, range(8, 12))
        take_shared(p, range(0, 4))
        matmul(t, p, range(12, 16))
        for s in range(2):
            take(p, 4 + 2 * s)
            take(p, 5 + 2 * s)
            matmul(t, p, range(16 + 4 * s, 18 + 4 * s))
            take_shared(p, (4 + 2 * s, 5 + 2 * s))
            matmul(t, p, range(18 + 4 * s, 20 + 4 * s))
        wait_a(t, range(24, 32))
        pltpu.make_async_copy(mbuf.at[p, pl.ds(0, DEV - 1)], mbuf.at[p, pl.ds(0, DEV - 1)], mrecv.at[p]).wait()
        pltpu.make_async_copy(mbuf.at[p, pl.ds(0, DEV - 1)], mbuf.at[p, pl.ds(0, DEV - 1)], msend.at[p]).wait()
        mass = jnp.sum(mbuf[p], axis=0)
        factor = factors[t]
        nodes = DEV * ROWS
        for h in range(2):
            take(p, 8 + 2 * h)
            matmul_half(p, (24, 25), h)
            take_shared(p, (8 + 2 * h,))
            matmul_half(p, (26, 27), h)
            take(p, 9 + 2 * h)
            matmul_half(p, (28, 29), h)
            take_shared(p, (9 + 2 * h,))
            sent = rbuf.at[p, h, pl.ds(0, 28 * TILE), :]
            pltpu.make_async_copy(sent, sent, ssem.at[p, h]).wait()
            lanes = pl.ds(h * HALF, HALF)
            row = (factor / nodes) * mass[:, h * HALF:(h + 1) * HALF]
            held = None
            for i in range(ROWS // SENT):
                for u in range(SENT // TILE):
                    j = i * (SENT // TILE) + u
                    rows = pl.ds(j * TILE, TILE)
                    total = acc[rows, lanes]
                    for c in (30, 31):
                        total += jnp.dot(abuf[slot_of(c), rows, :], rbuf[p, h, pl.ds(first(*order[c]), TILE), :], preferred_element_type=jnp.float32)
                    new = factor * total + (1.0 - factor) * tbuf[rows, lanes] + row
                    acc[rows, lanes] = new
                    rbuf[q, h, pl.ds(first(me, j), TILE), :] = new.astype(jnp.bfloat16)
                    part = mass_of(new, rows, h)
                    held = part if held is None else held + part

                @pl.when(t < sweeps - 1)
                def _():
                    send_x(q, i + 2 * h)
                    send_y(q, i + 2 * h)
                    share_own(q, 2 * i, h)
                    share_own(q, 2 * i + 1, h)
                    if i + h == 2:
                        for k in (4, 5):
                            send_x(q, k)
                            send_y(q, k)

            mbuf[q, me, :, lanes] = held

        @pl.when(t < sweeps - 1)
        def _():
            send_mass(q)


def solution(mesh):
    spec_rows = P(("batch", "row"), None)
    spec_vec = P(("batch", "row"))

    def local_sweeps(mat_rows, tele_rows, dang_rows, damping, start_rows):
        sweeps = damping.shape[0]
        hbm = pl.BlockSpec(memory_space=pl.ANY)
        return pl.pallas_call(
            functools.partial(kernel, sweeps),
            out_shape=pltpu.VMEM((ROWS, COLS), jnp.float32),
            in_specs=[hbm] * 5,
            out_specs=pl.BlockSpec(memory_space=pltpu.VMEM),
            scratch_shapes=[
                pltpu.SMEM((sweeps,), jnp.float32),
                pltpu.VMEM((2, 2, DEV * ROWS, HALF), jnp.bfloat16),
                pltpu.VMEM((len(KEPT) + RING, ROWS, TILE), jnp.bfloat16),
                pltpu.VMEM((ROWS, COLS), jnp.float32),
                pltpu.VMEM((ROWS, HALF), jnp.bfloat16),
                pltpu.VMEM((ROWS // 128, 128), jnp.int32),
                pltpu.VMEM((2, DEV, 1, COLS), jnp.float32),
                pltpu.SemaphoreType.DMA((len(KEPT) + RING,)),
                pltpu.SemaphoreType.DMA((7,)),
                pltpu.SemaphoreType.DMA((2, 2)),
                pltpu.SemaphoreType.DMA((2, 12)),
                pltpu.SemaphoreType.DMA((2, 12)),
                pltpu.SemaphoreType.DMA((2, 32)),
                pltpu.SemaphoreType.DMA((2,)),
                pltpu.SemaphoreType.DMA((2,)),
            ],
            compiler_params=pltpu.CompilerParams(collective_id=0, has_side_effects=True, vmem_limit_bytes=64880640),
            name="sweeps",
        )(mat_rows, tele_rows, dang_rows.reshape(ROWS // 128, 128), damping, start_rows)

    return jax.shard_map(local_sweeps, mesh=mesh, in_specs=(spec_rows, spec_rows, spec_vec, P(None), spec_rows), out_specs=spec_rows, check_vma=False)
```

```python
import functools

import jax
import jax.numpy as jnp
from jax import lax
from jax.experimental import pallas as pl
from jax.experimental.pallas import tpu as pltpu
from jax.sharding import PartitionSpec as P

MESH = pl.DeviceIdType.MESH

DEV = 8
ROWS = 2048
TILE = 512
HALF = 128
COLS = 256
KEPT = (0, 1, 2, 3, 14, 15, 24, 25, 26, 27, 28, 29, 30, 31)
STREAMED = tuple(c for c in range(32) if c not in KEPT)
RING = 6
MROWS = 1024
SENT = 1024

X_SLOTS = ((0, 0, 0), (0, 2, 0), (0, 0, 1), (0, 2, 1), (0, 1, 0), (0, 1, 1), (1, 1, 0), (1, 1, 1), (1, 3, 0), (0, 3, 0), (1, 3, 1), (0, 3, 1))
Y_SLOTS = ((0, 1, 0), (0, 3, 0), (0, 1, 1), (0, 3, 1), (0, 0, 0), (0, 0, 1), (1, 0, 0), (1, 0, 1), (1, 2, 0), (0, 2, 0), (1, 2, 1), (0, 2, 1))


def kernel(sweeps, mat, tele, dang, damp, start, acc, factors, rbuf, abuf, tbuf, dcol, draw, mbuf, asem, lsem, ssem, xsem, ysem, dsem, msend, mrecv):
    me = lax.axis_index("row")
    core = lax.rem(me, 2)
    xbit = lax.rem(lax.div(me, 2), 2)
    ybit = lax.div(me, 4)

    def device(xb, yb, cb):
        return yb * 4 + xb * 2 + cb

    xn, yn, pt = device(1 - xbit, ybit, core), device(xbit, 1 - ybit, core), device(xbit, ybit, 1 - core)
    dg = device(1 - xbit, 1 - ybit, core)
    pxn, pyn, pdg = device(1 - xbit, ybit, 1 - core), device(xbit, 1 - ybit, 1 - core), device(1 - xbit, 1 - ybit, 1 - core)

    order = [(me, j) for j in range(4)] + [(pt, j) for j in range(4)]
    order += [(xn, 0), (xn, 2), (yn, 1), (yn, 3), (pxn, 0), (pxn, 2), (pyn, 1), (pyn, 3)]
    order += [(xn, 1), (yn, 0), (pxn, 1), (pyn, 0), (dg, 1), (dg, 0), (pdg, 1), (pdg, 0)]
    order += [(dg, 3), (dg, 2), (pdg, 3), (pdg, 2), (xn, 3), (yn, 2), (pxn, 3), (pyn, 2)]

    def first(dv, j):
        return pl.multiple_of(dv * ROWS + j * TILE, TILE)

    def slot_of(c):
        return KEPT.index(c) if c in KEPT else len(KEPT) + STREAMED.index(c) % RING

    def load(c):
        dv, j = order[c]
        return pltpu.make_async_copy(mat.at[:, pl.ds(first(dv, j), TILE)], abuf.at[slot_of(c)], asem.at[slot_of(c)])

    def piece(p, dv, j, h):
        return rbuf.at[p, h, pl.ds(first(dv, j), TILE), :]

    def send(p, dv, j, h, to, recv):
        return pltpu.make_async_remote_copy(
            src_ref=piece(p, dv, j, h), dst_ref=piece(p, dv, j, h), send_sem=ssem.at[p, h], recv_sem=recv,
            device_id={"row": to}, device_id_type=MESH,
        )

    def arrived(p, dv, j, h, recv):
        pltpu.make_async_copy(piece(p, dv, j, h), piece(p, dv, j, h), recv).wait()

    def send_x(p, k):
        fwd, j, h = X_SLOTS[k]
        send(p, yn if fwd else me, j, h, xn, xsem.at[p, k]).start()

    def send_y(p, k):
        fwd, j, h = Y_SLOTS[k]
        send(p, xn if fwd else me, j, h, yn, ysem.at[p, k]).start()

    def share_own(p, j, h):
        send(p, me, j, h, pt, dsem.at[p, 2 * j + h]).start()

    def take(p, k):
        fwd, j, h = X_SLOTS[k]
        src = dg if fwd else xn
        arrived(p, src, j, h, xsem.at[p, k])
        send(p, src, j, h, pt, dsem.at[p, 8 + k]).start()
        fwd, j, h = Y_SLOTS[k]
        src = dg if fwd else yn
        arrived(p, src, j, h, ysem.at[p, k])
        send(p, src, j, h, pt, dsem.at[p, 20 + k]).start()

    def take_shared(p, ks):
        for k in ks:
            fwd, j, h = X_SLOTS[k]
            arrived(p, pdg if fwd else pxn, j, h, dsem.at[p, 8 + k])
            fwd, j, h = Y_SLOTS[k]
            arrived(p, pdg if fwd else pyn, j, h, dsem.at[p, 20 + k])

    def mass_of(values, rows, h):
        weighted = values * dcol[rows, :].astype(jnp.float32)
        return jnp.sum(weighted.reshape(-1, 8, HALF), axis=0).sum(axis=0, keepdims=True)

    def send_mass(p):
        for dx, dy, dc in [(a, b, c) for a in range(2) for b in range(2) for c in range(2)][1:]:
            to = device(lax.rem(xbit + dx, 2), lax.rem(ybit + dy, 2), lax.rem(core + dc, 2))
            pltpu.make_async_remote_copy(
                src_ref=mbuf.at[p, me], dst_ref=mbuf.at[p, me], send_sem=msend.at[p], recv_sem=mrecv.at[p],
                device_id={"row": to}, device_id_type=MESH,
            ).start()

    def wait_a(t, cs):
        for c in cs:
            if c in KEPT:
                @pl.when(t == 0)
                def _():
                    load(c).wait()
            else:
                load(c).wait()

    def refill(t, cs):
        for c in cs:
            if c in KEPT:
                continue
            later = STREAMED.index(c) + RING
            if later < len(STREAMED):
                load(STREAMED[later]).start()
            else:
                @pl.when(t < sweeps - 1)
                def _():
                    load(STREAMED[later - len(STREAMED)]).start()

    def wide(p, c):
        r = pl.ds(first(*order[c]), TILE)
        return jnp.concatenate([rbuf[p, 0, r, :], rbuf[p, 1, r, :]], axis=1)

    def matmul(t, p, cs, init=False):
        wait_a(t, cs)

        for i in range(ROWS // MROWS):
            rows = pl.ds(i * MROWS, MROWS)
            total = None
            for c in cs:
                part = jnp.dot(abuf[slot_of(c), rows, :], wide(p, c), preferred_element_type=jnp.float32)
                total = part if total is None else total + part
            acc[rows, :] = total if init else acc[rows, :] + total

        refill(t, cs)

    def matmul_half(p, cs, h):
        for i in range(ROWS // MROWS):
            rows = pl.ds(i * MROWS, MROWS)
            lanes = pl.ds(h * HALF, HALF)
            total = None
            for c in cs:
                part = jnp.dot(abuf[slot_of(c), rows, :], rbuf[p, h, pl.ds(first(*order[c]), TILE), :], preferred_element_type=jnp.float32)
                total = part if total is None else total + part
            acc[rows, lanes] += total

    barrier = pltpu.get_barrier_semaphore()
    for dx, dy, dc in [(a, b, c) for a in range(2) for b in range(2) for c in range(2)][1:]:
        to = device(lax.rem(xbit + dx, 2), lax.rem(ybit + dy, 2), lax.rem(core + dc, 2))
        pl.semaphore_signal(barrier, inc=1, device_id={"row": to}, device_id_type=MESH)
    own_rows = []
    for j in range(4):
        rows = pl.ds(j * TILE, TILE)
        own_rows.append(pltpu.make_async_copy(start.at[rows, :], acc.at[rows, :], lsem.at[3 + j]))
        own_rows[j].start()
    own_dang = pltpu.make_async_copy(dang, draw, lsem.at[0])
    own_dang.start()
    own_damp = pltpu.make_async_copy(damp, factors, lsem.at[1])
    own_damp.start()
    for c in sorted(KEPT + STREAMED[:RING]):
        load(c).start()
    own_tele = pltpu.make_async_copy(tele, tbuf, lsem.at[2])
    own_tele.start()
    for j in range(4):
        own_rows[j].wait()
        for h in range(2):
            rbuf[0, h, pl.ds(first(me, j), TILE), :] = acc[pl.ds(j * TILE, TILE), pl.ds(h * HALF, HALF)].astype(jnp.bfloat16)
        if j == 1:
            pl.semaphore_wait(barrier, DEV - 1)
            send_x(0, 0)
            send_y(0, 0)
    for k in range(1, 6):
        send_x(0, k)
        send_y(0, k)
    for h in range(2):
        for j in range(4):
            share_own(0, j, h)
    own_dang.wait()
    for i in range(ROWS // 128):
        line = jnp.broadcast_to(draw[pl.ds(i, 1), :].astype(jnp.float32), (128, 128))
        dcol[pl.ds(i * 128, 128), :] = jnp.transpose(line).astype(jnp.bfloat16)
    for h in range(2):
        total = None
        for j in range(4):
            rows = pl.ds(j * TILE, TILE)
            part = mass_of(acc[rows, pl.ds(h * HALF, HALF)], rows, h)
            total = part if total is None else total + part
        mbuf[0, me, :, pl.ds(h * HALF, HALF)] = total
    send_mass(0)
    own_tele.wait()
    own_damp.wait()

    @pl.loop(0, sweeps)
    def _(t):
        p = lax.rem(t, 2)
        q = 1 - p
        for j in range(4):
            for h in range(2):
                arrived(p, pt, j, h, dsem.at[p, 2 * j + h])
        matmul(t, p, range(0, 8), init=True)
        for k in range(3):
            take(p, k)
        for k in (6, 7, 8, 9):
            send_x(p, k)
            send_y(p, k)
        take(p, 3)
        for k in (10, 11):
            send_x(p, k)
            send_y(p, k)
        matmul(t, p, range(8, 12))
        take_shared(p, range(0, 4))
        matmul(t, p, range(12, 16))
        for s in range(2):
            take(p, 4 + 2 * s)
            take(p, 5 + 2 * s)
            matmul(t, p, range(16 + 4 * s, 18 + 4 * s))
            take_shared(p, (4 + 2 * s, 5 + 2 * s))
            matmul(t, p, range(18 + 4 * s, 20 + 4 * s))
        wait_a(t, range(24, 32))
        pltpu.make_async_copy(mbuf.at[p, pl.ds(0, DEV - 1)], mbuf.at[p, pl.ds(0, DEV - 1)], mrecv.at[p]).wait()
        pltpu.make_async_copy(mbuf.at[p, pl.ds(0, DEV - 1)], mbuf.at[p, pl.ds(0, DEV - 1)], msend.at[p]).wait()
        mass = jnp.sum(mbuf[p], axis=0)
        factor = factors[t]
        nodes = DEV * ROWS
        for h in range(2):
            take(p, 8 + 2 * h)
            matmul_half(p, (24, 25), h)
            take_shared(p, (8 + 2 * h,))
            matmul_half(p, (26, 27), h)
            take(p, 9 + 2 * h)
            matmul_half(p, (28, 29), h)
            take_shared(p, (9 + 2 * h,))
            sent = rbuf.at[p, h, pl.ds(0, 28 * TILE), :]
            pltpu.make_async_copy(sent, sent, ssem.at[p, h]).wait()
            lanes = pl.ds(h * HALF, HALF)
            row = (factor / nodes) * mass[:, h * HALF:(h + 1) * HALF]
            held = None
            for i in range(ROWS // SENT):
                for u in range(1):
                    j = 2 * i
                    rows = pl.ds(j * TILE, SENT)
                    total = None
                    for c in (30, 31):
                        part = jnp.dot(abuf[slot_of(c), rows, :], rbuf[p, h, pl.ds(first(*order[c]), TILE), :], preferred_element_type=jnp.float32)
                        total = part if total is None else total + part
                    total += acc[rows, lanes]
                    new = factor * total + (1.0 - factor) * tbuf[rows, lanes] + row
                    acc[rows, lanes] = new
                    rbuf[q, h, pl.ds(first(me, j), SENT), :] = new.astype(jnp.bfloat16)
                    part = mass_of(new, rows, h)
                    held = part if held is None else held + part

                @pl.when(t < sweeps - 1)
                def _():
                    send_x(q, i + 2 * h)
                    send_y(q, i + 2 * h)
                    share_own(q, 2 * i, h)
                    share_own(q, 2 * i + 1, h)
                    if i + h == 2:
                        for k in (4, 5):
                            send_x(q, k)
                            send_y(q, k)

            mbuf[q, me, :, lanes] = held

        @pl.when(t < sweeps - 1)
        def _():
            send_mass(q)


def solution(mesh):
    spec_rows = P(("batch", "row"), None)
    spec_vec = P(("batch", "row"))

    def local_sweeps(mat_rows, tele_rows, dang_rows, damping, start_rows):
        sweeps = damping.shape[0]
        hbm = pl.BlockSpec(memory_space=pl.ANY)
        return pl.pallas_call(
            functools.partial(kernel, sweeps),
            out_shape=pltpu.VMEM((ROWS, COLS), jnp.float32),
            in_specs=[hbm] * 5,
            out_specs=pl.BlockSpec(memory_space=pltpu.VMEM),
            scratch_shapes=[
                pltpu.SMEM((sweeps,), jnp.float32),
                pltpu.VMEM((2, 2, DEV * ROWS, HALF), jnp.bfloat16),
                pltpu.VMEM((len(KEPT) + RING, ROWS, TILE), jnp.bfloat16),
                pltpu.VMEM((ROWS, COLS), jnp.float32),
                pltpu.VMEM((ROWS, HALF), jnp.bfloat16),
                pltpu.VMEM((ROWS // 128, 128), jnp.int32),
                pltpu.VMEM((2, DEV, 1, COLS), jnp.float32),
                pltpu.SemaphoreType.DMA((len(KEPT) + RING,)),
                pltpu.SemaphoreType.DMA((7,)),
                pltpu.SemaphoreType.DMA((2, 2)),
                pltpu.SemaphoreType.DMA((2, 12)),
                pltpu.SemaphoreType.DMA((2, 12)),
                pltpu.SemaphoreType.DMA((2, 32)),
                pltpu.SemaphoreType.DMA((2,)),
                pltpu.SemaphoreType.DMA((2,)),
            ],
            compiler_params=pltpu.CompilerParams(collective_id=0, has_side_effects=True, vmem_limit_bytes=64880640),
            name="sweeps",
        )(mat_rows, tele_rows, dang_rows.reshape(ROWS // 128, 128), damping, start_rows)

    return jax.shard_map(local_sweeps, mesh=mesh, in_specs=(spec_rows, spec_rows, spec_vec, P(None), spec_rows), out_specs=spec_rows, check_vma=False)
```

```python
import functools

import jax
import jax.numpy as jnp
from jax import lax
from jax.experimental import pallas as pl
from jax.experimental.pallas import tpu as pltpu
from jax.sharding import PartitionSpec as P

MESH = pl.DeviceIdType.MESH

DEV = 8
ROWS = 2048
TILE = 512
HALF = 128
COLS = 256
KEPT = (0, 1, 2, 3, 14, 15, 24, 25, 26, 27, 28, 29, 30, 31)
STREAMED = tuple(c for c in range(32) if c not in KEPT)
RING = 6
MROWS = 1024
SENT = 1024

X_SLOTS = ((0, 0, 0), (0, 2, 0), (0, 0, 1), (0, 2, 1), (0, 1, 0), (0, 1, 1), (1, 1, 0), (1, 1, 1), (1, 3, 0), (0, 3, 0), (1, 3, 1), (0, 3, 1))
Y_SLOTS = ((0, 1, 0), (0, 3, 0), (0, 1, 1), (0, 3, 1), (0, 0, 0), (0, 0, 1), (1, 0, 0), (1, 0, 1), (1, 2, 0), (0, 2, 0), (1, 2, 1), (0, 2, 1))


def kernel(sweeps, mat, tele, dang, damp, start, acc, factors, rbuf, abuf, tbuf, dcol, draw, mbuf, asem, lsem, ssem, xsem, ysem, dsem, msend, mrecv):
    me = lax.axis_index("row")
    core = lax.rem(me, 2)
    xbit = lax.rem(lax.div(me, 2), 2)
    ybit = lax.div(me, 4)

    def device(xb, yb, cb):
        return yb * 4 + xb * 2 + cb

    xn, yn, pt = device(1 - xbit, ybit, core), device(xbit, 1 - ybit, core), device(xbit, ybit, 1 - core)
    dg = device(1 - xbit, 1 - ybit, core)
    pxn, pyn, pdg = device(1 - xbit, ybit, 1 - core), device(xbit, 1 - ybit, 1 - core), device(1 - xbit, 1 - ybit, 1 - core)

    order = [(me, j) for j in range(4)] + [(pt, j) for j in range(4)]
    order += [(xn, 0), (xn, 2), (yn, 1), (yn, 3), (pxn, 0), (pxn, 2), (pyn, 1), (pyn, 3)]
    order += [(xn, 1), (yn, 0), (pxn, 1), (pyn, 0), (dg, 1), (dg, 0), (pdg, 1), (pdg, 0)]
    order += [(dg, 3), (dg, 2), (pdg, 3), (pdg, 2), (xn, 3), (yn, 2), (pxn, 3), (pyn, 2)]

    def first(dv, j):
        return pl.multiple_of(dv * ROWS + j * TILE, TILE)

    def slot_of(c):
        return KEPT.index(c) if c in KEPT else len(KEPT) + STREAMED.index(c) % RING

    def load(c):
        dv, j = order[c]
        return pltpu.make_async_copy(mat.at[:, pl.ds(first(dv, j), TILE)], abuf.at[slot_of(c)], asem.at[slot_of(c)])

    def piece(p, dv, j, h):
        return rbuf.at[p, h, pl.ds(first(dv, j), TILE), :]

    def send(p, dv, j, h, to, recv):
        return pltpu.make_async_remote_copy(
            src_ref=piece(p, dv, j, h), dst_ref=piece(p, dv, j, h), send_sem=ssem.at[p, h], recv_sem=recv,
            device_id={"row": to}, device_id_type=MESH,
        )

    def arrived(p, dv, j, h, recv):
        pltpu.make_async_copy(piece(p, dv, j, h), piece(p, dv, j, h), recv).wait()

    def send_x(p, k):
        fwd, j, h = X_SLOTS[k]
        send(p, yn if fwd else me, j, h, xn, xsem.at[p, k]).start()

    def send_y(p, k):
        fwd, j, h = Y_SLOTS[k]
        send(p, xn if fwd else me, j, h, yn, ysem.at[p, k]).start()

    def share_own(p, j, h):
        send(p, me, j, h, pt, dsem.at[p, 2 * j + h]).start()

    def take(p, k):
        fwd, j, h = X_SLOTS[k]
        src = dg if fwd else xn
        arrived(p, src, j, h, xsem.at[p, k])
        send(p, src, j, h, pt, dsem.at[p, 8 + k]).start()
        fwd, j, h = Y_SLOTS[k]
        src = dg if fwd else yn
        arrived(p, src, j, h, ysem.at[p, k])
        send(p, src, j, h, pt, dsem.at[p, 20 + k]).start()

    def take_shared(p, ks):
        for k in ks:
            fwd, j, h = X_SLOTS[k]
            arrived(p, pdg if fwd else pxn, j, h, dsem.at[p, 8 + k])
            fwd, j, h = Y_SLOTS[k]
            arrived(p, pdg if fwd else pyn, j, h, dsem.at[p, 20 + k])

    def mass_of(values, rows, h):
        weighted = values * dcol[rows, :].astype(jnp.float32)
        return jnp.sum(weighted.reshape(-1, 8, HALF), axis=0).sum(axis=0, keepdims=True)

    def send_mass(p):
        for dx, dy, dc in [(a, b, c) for a in range(2) for b in range(2) for c in range(2)][1:]:
            to = device(lax.rem(xbit + dx, 2), lax.rem(ybit + dy, 2), lax.rem(core + dc, 2))
            pltpu.make_async_remote_copy(
                src_ref=mbuf.at[p, me], dst_ref=mbuf.at[p, me], send_sem=msend.at[p], recv_sem=mrecv.at[p],
                device_id={"row": to}, device_id_type=MESH,
            ).start()

    def wait_a(t, cs):
        for c in cs:
            if c in KEPT:
                @pl.when(t == 0)
                def _():
                    load(c).wait()
            else:
                load(c).wait()

    def refill(t, cs):
        for c in cs:
            if c in KEPT:
                continue
            later = STREAMED.index(c) + RING
            if later < len(STREAMED):
                load(STREAMED[later]).start()
            else:
                @pl.when(t < sweeps - 1)
                def _():
                    load(STREAMED[later - len(STREAMED)]).start()

    def wide(p, c):
        r = pl.ds(first(*order[c]), TILE)
        return jnp.concatenate([rbuf[p, 0, r, :], rbuf[p, 1, r, :]], axis=1)

    def matmul(t, p, cs, init=False):
        wait_a(t, cs)

        for i in range(ROWS // MROWS):
            rows = pl.ds(i * MROWS, MROWS)
            total = None
            for c in cs:
                part = jnp.dot(abuf[slot_of(c), rows, :], wide(p, c), preferred_element_type=jnp.float32)
                total = part if total is None else total + part
            acc[rows, :] = total if init else acc[rows, :] + total

        refill(t, cs)

    def matmul_half(p, cs, h):
        for i in range(ROWS // MROWS):
            rows = pl.ds(i * MROWS, MROWS)
            lanes = pl.ds(h * HALF, HALF)
            total = None
            for c in cs:
                part = jnp.dot(abuf[slot_of(c), rows, :], rbuf[p, h, pl.ds(first(*order[c]), TILE), :], preferred_element_type=jnp.float32)
                total = part if total is None else total + part
            acc[rows, lanes] += total

    barrier = pltpu.get_barrier_semaphore()
    for dx, dy, dc in [(a, b, c) for a in range(2) for b in range(2) for c in range(2)][1:]:
        to = device(lax.rem(xbit + dx, 2), lax.rem(ybit + dy, 2), lax.rem(core + dc, 2))
        pl.semaphore_signal(barrier, inc=1, device_id={"row": to}, device_id_type=MESH)
    own_rows = []
    for j in range(4):
        rows = pl.ds(j * TILE, TILE)
        own_rows.append(pltpu.make_async_copy(start.at[rows, :], acc.at[rows, :], lsem.at[3 + j]))
        own_rows[j].start()
    own_dang = pltpu.make_async_copy(dang, draw, lsem.at[0])
    own_dang.start()
    own_damp = pltpu.make_async_copy(damp, factors, lsem.at[1])
    own_damp.start()
    for c in sorted(KEPT + STREAMED[:RING]):
        load(c).start()
    own_tele = pltpu.make_async_copy(tele, tbuf, lsem.at[2])
    own_tele.start()
    for j in range(4):
        own_rows[j].wait()
        for h in range(2):
            rbuf[0, h, pl.ds(first(me, j), TILE), :] = acc[pl.ds(j * TILE, TILE), pl.ds(h * HALF, HALF)].astype(jnp.bfloat16)
        if j == 1:
            pl.semaphore_wait(barrier, DEV - 1)
            send_x(0, 0)
            send_y(0, 0)
    for k in range(1, 6):
        send_x(0, k)
        send_y(0, k)
    for h in range(2):
        for j in range(4):
            share_own(0, j, h)
    own_dang.wait()
    for i in range(ROWS // 128):
        line = jnp.broadcast_to(draw[pl.ds(i, 1), :].astype(jnp.float32), (128, 128))
        dcol[pl.ds(i * 128, 128), :] = jnp.transpose(line).astype(jnp.bfloat16)
    for h in range(2):
        total = None
        for j in range(4):
            rows = pl.ds(j * TILE, TILE)
            part = mass_of(acc[rows, pl.ds(h * HALF, HALF)], rows, h)
            total = part if total is None else total + part
        mbuf[0, me, :, pl.ds(h * HALF, HALF)] = total
    send_mass(0)
    own_tele.wait()
    own_damp.wait()

    @pl.loop(0, sweeps)
    def _(t):
        p = lax.rem(t, 2)
        q = 1 - p
        for j in range(4):
            for h in range(2):
                arrived(p, pt, j, h, dsem.at[p, 2 * j + h])
        matmul(t, p, range(0, 8), init=True)
        for k in range(3):
            take(p, k)
        for k in (6, 7, 8, 9):
            send_x(p, k)
            send_y(p, k)
        take(p, 3)
        for k in (10, 11):
            send_x(p, k)
            send_y(p, k)
        matmul(t, p, range(8, 12))
        take_shared(p, range(0, 4))
        matmul(t, p, range(12, 16))
        for s in range(2):
            take(p, 4 + 2 * s)
            take(p, 5 + 2 * s)
            matmul(t, p, range(16 + 4 * s, 18 + 4 * s))
            take_shared(p, (4 + 2 * s, 5 + 2 * s))
            matmul(t, p, range(18 + 4 * s, 20 + 4 * s))
        wait_a(t, range(24, 32))
        pltpu.make_async_copy(mbuf.at[p, pl.ds(0, DEV - 1)], mbuf.at[p, pl.ds(0, DEV - 1)], mrecv.at[p]).wait()
        pltpu.make_async_copy(mbuf.at[p, pl.ds(0, DEV - 1)], mbuf.at[p, pl.ds(0, DEV - 1)], msend.at[p]).wait()
        mass = jnp.sum(mbuf[p], axis=0)
        factor = factors[t]
        nodes = DEV * ROWS
        for h in range(2):
            take(p, 8 + 2 * h)
            matmul_half(p, (24, 25), h)
            take_shared(p, (8 + 2 * h,))
            matmul_half(p, (26, 27), h)
            take(p, 9 + 2 * h)
            matmul_half(p, (28, 29), h)
            take_shared(p, (9 + 2 * h,))
            lanes = pl.ds(h * HALF, HALF)
            row = (factor / nodes) * mass[:, h * HALF:(h + 1) * HALF]
            for i in range(ROWS // SENT):
                rows = pl.ds(i * SENT, SENT)
                total = None
                for c in (30, 31):
                    part = jnp.dot(abuf[slot_of(c), rows, :], rbuf[p, h, pl.ds(first(*order[c]), TILE), :], preferred_element_type=jnp.float32)
                    total = part if total is None else total + part
                total += acc[rows, lanes]
                new = factor * total + (1.0 - factor) * tbuf[rows, lanes] + row
                acc[rows, lanes] = new
                rbuf[q, h, pl.ds(first(me, 2 * i), SENT), :] = new.astype(jnp.bfloat16)

                if i == ROWS // SENT - 1:
                    sent = rbuf.at[p, h, pl.ds(0, 28 * TILE), :]
                    pltpu.make_async_copy(sent, sent, ssem.at[p, h]).wait()

                @pl.when(t < sweeps - 1)
                def _():
                    send_x(q, i + 2 * h)
                    send_y(q, i + 2 * h)
                    share_own(q, 2 * i, h)
                    share_own(q, 2 * i + 1, h)
                    if i + h == 2:
                        for k in (4, 5):
                            send_x(q, k)
                            send_y(q, k)


        @pl.when(t < sweeps - 1)
        def _():
            for h in range(2):
                lanes = pl.ds(h * HALF, HALF)
                held = None
                for j in range(4):
                    rows = pl.ds(j * TILE, TILE)
                    part = mass_of(acc[rows, lanes], rows, h)
                    held = part if held is None else held + part
                mbuf[q, me, :, lanes] = held
            send_mass(q)


def solution(mesh):
    spec_rows = P(("batch", "row"), None)
    spec_vec = P(("batch", "row"))

    def local_sweeps(mat_rows, tele_rows, dang_rows, damping, start_rows):
        sweeps = damping.shape[0]
        hbm = pl.BlockSpec(memory_space=pl.ANY)
        return pl.pallas_call(
            functools.partial(kernel, sweeps),
            out_shape=pltpu.VMEM((ROWS, COLS), jnp.float32),
            in_specs=[hbm] * 5,
            out_specs=pl.BlockSpec(memory_space=pltpu.VMEM),
            scratch_shapes=[
                pltpu.SMEM((sweeps,), jnp.float32),
                pltpu.VMEM((2, 2, DEV * ROWS, HALF), jnp.bfloat16),
                pltpu.VMEM((len(KEPT) + RING, ROWS, TILE), jnp.bfloat16),
                pltpu.VMEM((ROWS, COLS), jnp.float32),
                pltpu.VMEM((ROWS, HALF), jnp.bfloat16),
                pltpu.VMEM((ROWS // 128, 128), jnp.int32),
                pltpu.VMEM((2, DEV, 1, COLS), jnp.float32),
                pltpu.SemaphoreType.DMA((len(KEPT) + RING,)),
                pltpu.SemaphoreType.DMA((7,)),
                pltpu.SemaphoreType.DMA((2, 2)),
                pltpu.SemaphoreType.DMA((2, 12)),
                pltpu.SemaphoreType.DMA((2, 12)),
                pltpu.SemaphoreType.DMA((2, 32)),
                pltpu.SemaphoreType.DMA((2,)),
                pltpu.SemaphoreType.DMA((2,)),
            ],
            compiler_params=pltpu.CompilerParams(collective_id=0, has_side_effects=True, vmem_limit_bytes=64880640),
            name="sweeps",
        )(mat_rows, tele_rows, dang_rows.reshape(ROWS // 128, 128), damping, start_rows)

    return jax.shard_map(local_sweeps, mesh=mesh, in_specs=(spec_rows, spec_rows, spec_vec, P(None), spec_rows), out_specs=spec_rows, check_vma=False)
```

```python
import functools

import jax
import jax.numpy as jnp
from jax import lax
from jax.experimental import pallas as pl
from jax.experimental.pallas import tpu as pltpu
from jax.sharding import PartitionSpec as P

MESH = pl.DeviceIdType.MESH

DEV = 8
ROWS = 2048
TILE = 512
HALF = 128
COLS = 256
KEPT = (0, 1, 2, 3, 14, 15, 24, 25, 26, 27, 28, 29, 30, 31)
STREAMED = tuple(c for c in range(32) if c not in KEPT)
RING = 6
MROWS = 1024
SENT = 1024

X_SLOTS = ((0, 0, 0), (0, 2, 0), (0, 0, 1), (0, 2, 1), (0, 1, 0), (0, 1, 1), (1, 1, 0), (1, 1, 1), (1, 3, 0), (0, 3, 0), (1, 3, 1), (0, 3, 1))
Y_SLOTS = ((0, 1, 0), (0, 3, 0), (0, 1, 1), (0, 3, 1), (0, 0, 0), (0, 0, 1), (1, 0, 0), (1, 0, 1), (1, 2, 0), (0, 2, 0), (1, 2, 1), (0, 2, 1))


def kernel(sweeps, mat, tele, dang, damp, start, acc, factors, rbuf, abuf, tbuf, dcol, draw, mbuf, asem, lsem, ssem, xsem, ysem, dsem, msend, mrecv):
    me = lax.axis_index("row")
    core = lax.rem(me, 2)
    xbit = lax.rem(lax.div(me, 2), 2)
    ybit = lax.div(me, 4)

    def device(xb, yb, cb):
        return yb * 4 + xb * 2 + cb

    xn, yn, pt = device(1 - xbit, ybit, core), device(xbit, 1 - ybit, core), device(xbit, ybit, 1 - core)
    dg = device(1 - xbit, 1 - ybit, core)
    pxn, pyn, pdg = device(1 - xbit, ybit, 1 - core), device(xbit, 1 - ybit, 1 - core), device(1 - xbit, 1 - ybit, 1 - core)

    order = [(me, j) for j in range(4)] + [(pt, j) for j in range(4)]
    order += [(xn, 0), (xn, 2), (yn, 1), (yn, 3), (pxn, 0), (pxn, 2), (pyn, 1), (pyn, 3)]
    order += [(xn, 1), (yn, 0), (pxn, 1), (pyn, 0), (dg, 1), (dg, 0), (pdg, 1), (pdg, 0)]
    order += [(dg, 3), (dg, 2), (pdg, 3), (pdg, 2), (xn, 3), (yn, 2), (pxn, 3), (pyn, 2)]

    def first(dv, j):
        return pl.multiple_of(dv * ROWS + j * TILE, TILE)

    def slot_of(c):
        return KEPT.index(c) if c in KEPT else len(KEPT) + STREAMED.index(c) % RING

    def load(c):
        dv, j = order[c]
        return pltpu.make_async_copy(mat.at[:, pl.ds(first(dv, j), TILE)], abuf.at[slot_of(c)], asem.at[slot_of(c)])

    def piece(p, dv, j, h):
        return rbuf.at[p, h, pl.ds(first(dv, j), TILE), :]

    def send(p, dv, j, h, to, recv):
        return pltpu.make_async_remote_copy(
            src_ref=piece(p, dv, j, h), dst_ref=piece(p, dv, j, h), send_sem=ssem.at[p, h], recv_sem=recv,
            device_id={"row": to}, device_id_type=MESH,
        )

    def arrived(p, dv, j, h, recv):
        pltpu.make_async_copy(piece(p, dv, j, h), piece(p, dv, j, h), recv).wait()

    def send_x(p, k):
        fwd, j, h = X_SLOTS[k]
        send(p, yn if fwd else me, j, h, xn, xsem.at[p, k]).start()

    def send_y(p, k):
        fwd, j, h = Y_SLOTS[k]
        send(p, xn if fwd else me, j, h, yn, ysem.at[p, k]).start()

    def share_own(p, j, h):
        send(p, me, j, h, pt, dsem.at[p, 2 * j + h]).start()

    def take(p, k):
        fwd, j, h = X_SLOTS[k]
        src = dg if fwd else xn
        arrived(p, src, j, h, xsem.at[p, k])
        send(p, src, j, h, pt, dsem.at[p, 8 + k]).start()
        fwd, j, h = Y_SLOTS[k]
        src = dg if fwd else yn
        arrived(p, src, j, h, ysem.at[p, k])
        send(p, src, j, h, pt, dsem.at[p, 20 + k]).start()

    def take_shared(p, ks):
        for k in ks:
            fwd, j, h = X_SLOTS[k]
            arrived(p, pdg if fwd else pxn, j, h, dsem.at[p, 8 + k])
            fwd, j, h = Y_SLOTS[k]
            arrived(p, pdg if fwd else pyn, j, h, dsem.at[p, 20 + k])

    def mass_of(values, rows, h):
        total = None
        for u in range(TILE // 128):
            line = rows.start // 128 + u
            part = values[u * 128:(u + 1) * 128] * dcol[:, line:line + 1]
            part = jnp.sum(part.reshape(-1, 8, HALF), axis=0)
            total = part if total is None else total + part
        return jnp.sum(total, axis=0, keepdims=True)

    def send_mass(p):
        for dx, dy, dc in [(a, b, c) for a in range(2) for b in range(2) for c in range(2)][1:]:
            to = device(lax.rem(xbit + dx, 2), lax.rem(ybit + dy, 2), lax.rem(core + dc, 2))
            pltpu.make_async_remote_copy(
                src_ref=mbuf.at[p, me], dst_ref=mbuf.at[p, me], send_sem=msend.at[p], recv_sem=mrecv.at[p],
                device_id={"row": to}, device_id_type=MESH,
            ).start()

    def wait_a(t, cs):
        for c in cs:
            if c in KEPT:
                @pl.when(t == 0)
                def _():
                    load(c).wait()
            else:
                load(c).wait()

    def refill(t, cs):
        for c in cs:
            if c in KEPT:
                continue
            later = STREAMED.index(c) + RING
            if later < len(STREAMED):
                load(STREAMED[later]).start()
            else:
                @pl.when(t < sweeps - 1)
                def _():
                    load(STREAMED[later - len(STREAMED)]).start()

    def wide(p, c):
        r = pl.ds(first(*order[c]), TILE)
        return jnp.concatenate([rbuf[p, 0, r, :], rbuf[p, 1, r, :]], axis=1)

    def matmul(t, p, cs, init=False):
        wait_a(t, cs)

        for i in range(ROWS // MROWS):
            rows = pl.ds(i * MROWS, MROWS)
            total = None
            for c in cs:
                part = jnp.dot(abuf[slot_of(c), rows, :], wide(p, c), preferred_element_type=jnp.float32)
                total = part if total is None else total + part
            acc[rows, :] = total if init else acc[rows, :] + total

        refill(t, cs)

    def matmul_half(p, cs, h):
        for i in range(ROWS // MROWS):
            rows = pl.ds(i * MROWS, MROWS)
            lanes = pl.ds(h * HALF, HALF)
            total = None
            for c in cs:
                part = jnp.dot(abuf[slot_of(c), rows, :], rbuf[p, h, pl.ds(first(*order[c]), TILE), :], preferred_element_type=jnp.float32)
                total = part if total is None else total + part
            acc[rows, lanes] += total

    barrier = pltpu.get_barrier_semaphore()
    for dx, dy, dc in [(a, b, c) for a in range(2) for b in range(2) for c in range(2)][1:]:
        to = device(lax.rem(xbit + dx, 2), lax.rem(ybit + dy, 2), lax.rem(core + dc, 2))
        pl.semaphore_signal(barrier, inc=1, device_id={"row": to}, device_id_type=MESH)
    own_rows = []
    for j in range(4):
        rows = pl.ds(j * TILE, TILE)
        own_rows.append(pltpu.make_async_copy(start.at[rows, :], acc.at[rows, :], lsem.at[3 + j]))
        own_rows[j].start()
    own_dang = pltpu.make_async_copy(dang, draw, lsem.at[0])
    own_dang.start()
    own_damp = pltpu.make_async_copy(damp, factors, lsem.at[1])
    own_damp.start()
    for c in sorted(KEPT + STREAMED[:RING]):
        load(c).start()
    own_tele = pltpu.make_async_copy(tele, tbuf, lsem.at[2])
    own_tele.start()
    for j in range(4):
        own_rows[j].wait()
        for h in range(2):
            rbuf[0, h, pl.ds(first(me, j), TILE), :] = acc[pl.ds(j * TILE, TILE), pl.ds(h * HALF, HALF)].astype(jnp.bfloat16)
        if j == 1:
            pl.semaphore_wait(barrier, DEV - 1)
            send_x(0, 0)
            send_y(0, 0)
    for k in range(1, 6):
        send_x(0, k)
        send_y(0, k)
    for h in range(2):
        for j in range(4):
            share_own(0, j, h)
    own_dang.wait()
    lines = jnp.concatenate([draw[...].astype(jnp.float32), jnp.zeros((128 - ROWS // 128, 128), jnp.float32)], axis=0)
    dcol[...] = jnp.transpose(lines)
    for h in range(2):
        total = None
        for j in range(4):
            rows = pl.ds(j * TILE, TILE)
            part = mass_of(acc[rows, pl.ds(h * HALF, HALF)], rows, h)
            total = part if total is None else total + part
        mbuf[0, me, :, pl.ds(h * HALF, HALF)] = total
    send_mass(0)
    own_tele.wait()
    own_damp.wait()

    @pl.loop(0, sweeps)
    def _(t):
        p = lax.rem(t, 2)
        q = 1 - p
        for j in range(4):
            for h in range(2):
                arrived(p, pt, j, h, dsem.at[p, 2 * j + h])
        matmul(t, p, range(0, 8), init=True)
        for k in range(3):
            take(p, k)
        for k in (6, 7, 8, 9):
            send_x(p, k)
            send_y(p, k)
        take(p, 3)
        for k in (10, 11):
            send_x(p, k)
            send_y(p, k)
        matmul(t, p, range(8, 12))
        take_shared(p, range(0, 4))
        matmul(t, p, range(12, 16))
        for s in range(2):
            take(p, 4 + 2 * s)
            take(p, 5 + 2 * s)
            matmul(t, p, range(16 + 4 * s, 18 + 4 * s))
            take_shared(p, (4 + 2 * s, 5 + 2 * s))
            matmul(t, p, range(18 + 4 * s, 20 + 4 * s))
        wait_a(t, range(24, 32))
        pltpu.make_async_copy(mbuf.at[p, pl.ds(0, DEV - 1)], mbuf.at[p, pl.ds(0, DEV - 1)], mrecv.at[p]).wait()
        pltpu.make_async_copy(mbuf.at[p, pl.ds(0, DEV - 1)], mbuf.at[p, pl.ds(0, DEV - 1)], msend.at[p]).wait()
        mass = jnp.sum(mbuf[p], axis=0)
        factor = factors[t]
        nodes = DEV * ROWS
        for h in range(2):
            take(p, 8 + 2 * h)
            matmul_half(p, (24, 25), h)
            take_shared(p, (8 + 2 * h,))
            matmul_half(p, (26, 27), h)
            take(p, 9 + 2 * h)
            matmul_half(p, (28, 29), h)
            take_shared(p, (9 + 2 * h,))
            lanes = pl.ds(h * HALF, HALF)
            row = (factor / nodes) * mass[:, h * HALF:(h + 1) * HALF]
            for i in range(ROWS // SENT):
                for j in (2 * i, 2 * i + 1):
                    rows = pl.ds(j * TILE, TILE)
                    total = None
                    for c in (30, 31):
                        part = jnp.dot(abuf[slot_of(c), rows, :], rbuf[p, h, pl.ds(first(*order[c]), TILE), :], preferred_element_type=jnp.float32)
                        total = part if total is None else total + part
                    total += acc[rows, lanes]
                    new = factor * total + (1.0 - factor) * tbuf[rows, lanes] + row
                    acc[rows, lanes] = new
                    rbuf[q, h, pl.ds(first(me, j), TILE), :] = new.astype(jnp.bfloat16)

                if i == ROWS // SENT - 1:
                    sent = rbuf.at[p, h, pl.ds(0, 28 * TILE), :]
                    pltpu.make_async_copy(sent, sent, ssem.at[p, h]).wait()

                @pl.when(t < sweeps - 1)
                def _():
                    send_x(q, i + 2 * h)
                    send_y(q, i + 2 * h)
                    share_own(q, 2 * i, h)
                    share_own(q, 2 * i + 1, h)
                    if i + h == 2:
                        for k in (4, 5):
                            send_x(q, k)
                            send_y(q, k)


        @pl.when(t < sweeps - 1)
        def _():
            for h in range(2):
                lanes = pl.ds(h * HALF, HALF)
                held = None
                for j in range(4):
                    rows = pl.ds(j * TILE, TILE)
                    part = mass_of(acc[rows, lanes], rows, h)
                    held = part if held is None else held + part
                mbuf[q, me, :, lanes] = held
            send_mass(q)


def solution(mesh):
    spec_rows = P(("batch", "row"), None)
    spec_vec = P(("batch", "row"))

    def local_sweeps(mat_rows, tele_rows, dang_rows, damping, start_rows):
        sweeps = damping.shape[0]
        hbm = pl.BlockSpec(memory_space=pl.ANY)
        return pl.pallas_call(
            functools.partial(kernel, sweeps),
            out_shape=pltpu.VMEM((ROWS, COLS), jnp.float32),
            in_specs=[hbm] * 5,
            out_specs=pl.BlockSpec(memory_space=pltpu.VMEM),
            scratch_shapes=[
                pltpu.SMEM((sweeps,), jnp.float32),
                pltpu.VMEM((2, 2, DEV * ROWS, HALF), jnp.bfloat16),
                pltpu.VMEM((len(KEPT) + RING, ROWS, TILE), jnp.bfloat16),
                pltpu.VMEM((ROWS, COLS), jnp.float32),
                pltpu.VMEM((128, 128), jnp.float32),
                pltpu.VMEM((ROWS // 128, 128), jnp.int32),
                pltpu.VMEM((2, DEV, 1, COLS), jnp.float32),
                pltpu.SemaphoreType.DMA((len(KEPT) + RING,)),
                pltpu.SemaphoreType.DMA((7,)),
                pltpu.SemaphoreType.DMA((2, 2)),
                pltpu.SemaphoreType.DMA((2, 12)),
                pltpu.SemaphoreType.DMA((2, 12)),
                pltpu.SemaphoreType.DMA((2, 32)),
                pltpu.SemaphoreType.DMA((2,)),
                pltpu.SemaphoreType.DMA((2,)),
            ],
            compiler_params=pltpu.CompilerParams(collective_id=0, has_side_effects=True, vmem_limit_bytes=64946176),
            name="sweeps",
        )(mat_rows, tele_rows, dang_rows.reshape(ROWS // 128, 128), damping, start_rows)

    return jax.shard_map(local_sweeps, mesh=mesh, in_specs=(spec_rows, spec_rows, spec_vec, P(None), spec_rows), out_specs=spec_rows, check_vma=False)
```

```python
import functools

import jax
import jax.numpy as jnp
from jax import lax
from jax.experimental import pallas as pl
from jax.experimental.pallas import tpu as pltpu
from jax.sharding import PartitionSpec as P

MESH = pl.DeviceIdType.MESH

DEV = 8
ROWS = 2048
TILE = 512
HALF = 128
COLS = 256
KEPT = (0, 1, 2, 3, 14, 15, 24, 25, 26, 27, 28, 29, 30, 31)
STREAMED = tuple(c for c in range(32) if c not in KEPT)
RING = 6
MROWS = 1024
SENT = 1024

X_SLOTS = ((0, 0, 0), (0, 2, 0), (0, 0, 1), (0, 2, 1), (0, 1, 0), (0, 1, 1), (1, 1, 0), (1, 1, 1), (1, 3, 0), (0, 3, 0), (1, 3, 1), (0, 3, 1))
Y_SLOTS = ((0, 1, 0), (0, 3, 0), (0, 1, 1), (0, 3, 1), (0, 0, 0), (0, 0, 1), (1, 0, 0), (1, 0, 1), (1, 2, 0), (0, 2, 0), (1, 2, 1), (0, 2, 1))


def kernel(sweeps, mat, tele, dang, damp, start, acc, factors, rbuf, abuf, tbuf, dcol, draw, mbuf, asem, lsem, ssem, xsem, ysem, dsem, msend, mrecv):
    me = lax.axis_index("row")
    core = lax.rem(me, 2)
    xbit = lax.rem(lax.div(me, 2), 2)
    ybit = lax.div(me, 4)

    def device(xb, yb, cb):
        return yb * 4 + xb * 2 + cb

    xn, yn, pt = device(1 - xbit, ybit, core), device(xbit, 1 - ybit, core), device(xbit, ybit, 1 - core)
    dg = device(1 - xbit, 1 - ybit, core)
    pxn, pyn, pdg = device(1 - xbit, ybit, 1 - core), device(xbit, 1 - ybit, 1 - core), device(1 - xbit, 1 - ybit, 1 - core)

    order = [(me, j) for j in range(4)] + [(pt, j) for j in range(4)]
    order += [(xn, 0), (xn, 2), (yn, 1), (yn, 3), (pxn, 0), (pxn, 2), (pyn, 1), (pyn, 3)]
    order += [(xn, 1), (yn, 0), (pxn, 1), (pyn, 0), (dg, 1), (dg, 0), (pdg, 1), (pdg, 0)]
    order += [(dg, 3), (dg, 2), (pdg, 3), (pdg, 2), (xn, 3), (yn, 2), (pxn, 3), (pyn, 2)]

    def first(dv, j):
        return pl.multiple_of(dv * ROWS + j * TILE, TILE)

    def slot_of(c):
        return KEPT.index(c) if c in KEPT else len(KEPT) + STREAMED.index(c) % RING

    def load(c):
        dv, j = order[c]
        return pltpu.make_async_copy(mat.at[:, pl.ds(first(dv, j), TILE)], abuf.at[slot_of(c)], asem.at[slot_of(c)])

    def piece(p, dv, j, h):
        return rbuf.at[p, h, pl.ds(first(dv, j), TILE), :]

    def send(p, dv, j, h, to, recv):
        return pltpu.make_async_remote_copy(
            src_ref=piece(p, dv, j, h), dst_ref=piece(p, dv, j, h), send_sem=ssem.at[p, h], recv_sem=recv,
            device_id={"row": to}, device_id_type=MESH,
        )

    def arrived(p, dv, j, h, recv):
        pltpu.make_async_copy(piece(p, dv, j, h), piece(p, dv, j, h), recv).wait()

    def send_x(p, k):
        fwd, j, h = X_SLOTS[k]
        send(p, yn if fwd else me, j, h, xn, xsem.at[p, k]).start()

    def send_y(p, k):
        fwd, j, h = Y_SLOTS[k]
        send(p, xn if fwd else me, j, h, yn, ysem.at[p, k]).start()

    def share_own(p, j, h):
        send(p, me, j, h, pt, dsem.at[p, 2 * j + h]).start()

    def take(p, k):
        fwd, j, h = X_SLOTS[k]
        src = dg if fwd else xn
        arrived(p, src, j, h, xsem.at[p, k])
        send(p, src, j, h, pt, dsem.at[p, 8 + k]).start()
        fwd, j, h = Y_SLOTS[k]
        src = dg if fwd else yn
        arrived(p, src, j, h, ysem.at[p, k])
        send(p, src, j, h, pt, dsem.at[p, 20 + k]).start()

    def take_shared(p, ks):
        for k in ks:
            fwd, j, h = X_SLOTS[k]
            arrived(p, pdg if fwd else pxn, j, h, dsem.at[p, 8 + k])
            fwd, j, h = Y_SLOTS[k]
            arrived(p, pdg if fwd else pyn, j, h, dsem.at[p, 20 + k])

    def mass_of(values, rows, h):
        total = None
        for u in range(TILE // 128):
            line = rows.start // 128 + u
            part = values[u * 128:(u + 1) * 128] * dcol[:, line:line + 1]
            part = jnp.sum(part.reshape(-1, 8, HALF), axis=0)
            total = part if total is None else total + part
        return jnp.sum(total, axis=0, keepdims=True)

    def send_mass(p):
        for dx, dy, dc in [(a, b, c) for a in range(2) for b in range(2) for c in range(2)][1:]:
            to = device(lax.rem(xbit + dx, 2), lax.rem(ybit + dy, 2), lax.rem(core + dc, 2))
            pltpu.make_async_remote_copy(
                src_ref=mbuf.at[p, me], dst_ref=mbuf.at[p, me], send_sem=msend.at[p], recv_sem=mrecv.at[p],
                device_id={"row": to}, device_id_type=MESH,
            ).start()

    def wait_a(t, cs):
        for c in cs:
            if c in KEPT:
                @pl.when(t == 0)
                def _():
                    load(c).wait()
            else:
                load(c).wait()

    def refill(t, cs):
        for c in cs:
            if c in KEPT:
                continue
            later = STREAMED.index(c) + RING
            if later < len(STREAMED):
                load(STREAMED[later]).start()
            else:
                @pl.when(t < sweeps - 1)
                def _():
                    load(STREAMED[later - len(STREAMED)]).start()

    def wide(p, c):
        r = pl.ds(first(*order[c]), TILE)
        return jnp.concatenate([rbuf[p, 0, r, :], rbuf[p, 1, r, :]], axis=1)

    def matmul(t, p, cs, init=False):
        wait_a(t, cs)

        for i in range(ROWS // MROWS):
            rows = pl.ds(i * MROWS, MROWS)
            total = None
            for c in cs:
                part = jnp.dot(abuf[slot_of(c), rows, :], wide(p, c), preferred_element_type=jnp.float32)
                total = part if total is None else total + part
            acc[rows, :] = total if init else acc[rows, :] + total

        refill(t, cs)

    def matmul_half(p, cs, h):
        for i in range(ROWS // MROWS):
            rows = pl.ds(i * MROWS, MROWS)
            lanes = pl.ds(h * HALF, HALF)
            total = None
            for c in cs:
                part = jnp.dot(abuf[slot_of(c), rows, :], rbuf[p, h, pl.ds(first(*order[c]), TILE), :], preferred_element_type=jnp.float32)
                total = part if total is None else total + part
            acc[rows, lanes] += total

    barrier = pltpu.get_barrier_semaphore()
    for dx, dy, dc in [(a, b, c) for a in range(2) for b in range(2) for c in range(2)][1:]:
        to = device(lax.rem(xbit + dx, 2), lax.rem(ybit + dy, 2), lax.rem(core + dc, 2))
        pl.semaphore_signal(barrier, inc=1, device_id={"row": to}, device_id_type=MESH)
    own_rows = []
    for j in range(4):
        rows = pl.ds(j * TILE, TILE)
        own_rows.append(pltpu.make_async_copy(start.at[rows, :], acc.at[rows, :], lsem.at[3 + j]))
        own_rows[j].start()
    own_dang = pltpu.make_async_copy(dang, draw, lsem.at[0])
    own_dang.start()
    own_damp = pltpu.make_async_copy(damp, factors, lsem.at[1])
    own_damp.start()
    for c in sorted(KEPT + STREAMED[:RING]):
        load(c).start()
    own_tele = pltpu.make_async_copy(tele, tbuf, lsem.at[2])
    own_tele.start()
    for j in range(4):
        own_rows[j].wait()
        for h in range(2):
            rbuf[0, h, pl.ds(first(me, j), TILE), :] = acc[pl.ds(j * TILE, TILE), pl.ds(h * HALF, HALF)].astype(jnp.bfloat16)
        if j == 1:
            pl.semaphore_wait(barrier, DEV - 1)
            send_x(0, 0)
            send_y(0, 0)
    for k in range(1, 6):
        send_x(0, k)
        send_y(0, k)
    for h in range(2):
        for j in range(4):
            share_own(0, j, h)
    own_dang.wait()
    lines = jnp.concatenate([draw[...].astype(jnp.float32), jnp.zeros((128 - ROWS // 128, 128), jnp.float32)], axis=0)
    dcol[...] = jnp.transpose(lines)
    for h in range(2):
        total = None
        for j in range(4):
            rows = pl.ds(j * TILE, TILE)
            part = mass_of(acc[rows, pl.ds(h * HALF, HALF)], rows, h)
            total = part if total is None else total + part
        mbuf[0, me, :, pl.ds(h * HALF, HALF)] = total
    send_mass(0)
    own_tele.wait()
    own_damp.wait()

    @pl.loop(0, sweeps)
    def _(t):
        p = lax.rem(t, 2)
        q = 1 - p
        for j in range(4):
            for h in range(2):
                arrived(p, pt, j, h, dsem.at[p, 2 * j + h])
        matmul(t, p, range(0, 8), init=True)
        for k in range(3):
            take(p, k)
        for k in (6, 7, 8, 9):
            send_x(p, k)
            send_y(p, k)
        take(p, 3)
        for k in (10, 11):
            send_x(p, k)
            send_y(p, k)
        matmul(t, p, range(8, 12))
        take_shared(p, range(0, 4))
        matmul(t, p, range(12, 16))
        for s in range(2):
            take(p, 4 + 2 * s)
            take(p, 5 + 2 * s)
            matmul(t, p, range(16 + 4 * s, 18 + 4 * s))
            take_shared(p, (4 + 2 * s, 5 + 2 * s))
            matmul(t, p, range(18 + 4 * s, 20 + 4 * s))
        wait_a(t, range(24, 32))
        pltpu.make_async_copy(mbuf.at[p, pl.ds(0, DEV - 1)], mbuf.at[p, pl.ds(0, DEV - 1)], mrecv.at[p]).wait()
        pltpu.make_async_copy(mbuf.at[p, pl.ds(0, DEV - 1)], mbuf.at[p, pl.ds(0, DEV - 1)], msend.at[p]).wait()
        mass = jnp.sum(mbuf[p], axis=0)
        factor = factors[t]
        nodes = DEV * ROWS
        for h in range(2):
            take(p, 8 + 2 * h)
            matmul_half(p, (24, 25), h)
            take_shared(p, (8 + 2 * h,))
            matmul_half(p, (26, 27), h)
            take(p, 9 + 2 * h)
            matmul_half(p, (28, 29), h)
            take_shared(p, (9 + 2 * h,))
            lanes = pl.ds(h * HALF, HALF)
            row = (factor / nodes) * mass[:, h * HALF:(h + 1) * HALF]
            for i in range(ROWS // SENT):
                rows = pl.ds(i * SENT, SENT)
                parts = [jnp.dot(abuf[slot_of(c), rows, :], rbuf[p, h, pl.ds(first(*order[c]), TILE), :], preferred_element_type=jnp.float32) for c in (30, 31)]
                new = factor * (acc[rows, lanes] + parts[0]) + factor * parts[1] + (1.0 - factor) * tbuf[rows, lanes] + row
                acc[rows, lanes] = new
                rbuf[q, h, pl.ds(first(me, 2 * i), SENT), :] = new.astype(jnp.bfloat16)

                if i == ROWS // SENT - 1:
                    sent = rbuf.at[p, h, pl.ds(0, 28 * TILE), :]
                    pltpu.make_async_copy(sent, sent, ssem.at[p, h]).wait()

                @pl.when(t < sweeps - 1)
                def _():
                    send_x(q, i + 2 * h)
                    send_y(q, i + 2 * h)
                    share_own(q, 2 * i, h)
                    share_own(q, 2 * i + 1, h)
                    if i + h == 2:
                        for k in (4, 5):
                            send_x(q, k)
                            send_y(q, k)


        @pl.when(t < sweeps - 1)
        def _():
            for h in range(2):
                lanes = pl.ds(h * HALF, HALF)
                held = None
                for j in range(4):
                    rows = pl.ds(j * TILE, TILE)
                    part = mass_of(acc[rows, lanes], rows, h)
                    held = part if held is None else held + part
                mbuf[q, me, :, lanes] = held
            send_mass(q)


def solution(mesh):
    spec_rows = P(("batch", "row"), None)
    spec_vec = P(("batch", "row"))

    def local_sweeps(mat_rows, tele_rows, dang_rows, damping, start_rows):
        sweeps = damping.shape[0]
        hbm = pl.BlockSpec(memory_space=pl.ANY)
        return pl.pallas_call(
            functools.partial(kernel, sweeps),
            out_shape=pltpu.VMEM((ROWS, COLS), jnp.float32),
            in_specs=[hbm] * 5,
            out_specs=pl.BlockSpec(memory_space=pltpu.VMEM),
            scratch_shapes=[
                pltpu.SMEM((sweeps,), jnp.float32),
                pltpu.VMEM((2, 2, DEV * ROWS, HALF), jnp.bfloat16),
                pltpu.VMEM((len(KEPT) + RING, ROWS, TILE), jnp.bfloat16),
                pltpu.VMEM((ROWS, COLS), jnp.float32),
                pltpu.VMEM((128, 128), jnp.float32),
                pltpu.VMEM((ROWS // 128, 128), jnp.int32),
                pltpu.VMEM((2, DEV, 1, COLS), jnp.float32),
                pltpu.SemaphoreType.DMA((len(KEPT) + RING,)),
                pltpu.SemaphoreType.DMA((7,)),
                pltpu.SemaphoreType.DMA((2, 2)),
                pltpu.SemaphoreType.DMA((2, 12)),
                pltpu.SemaphoreType.DMA((2, 12)),
                pltpu.SemaphoreType.DMA((2, 32)),
                pltpu.SemaphoreType.DMA((2,)),
                pltpu.SemaphoreType.DMA((2,)),
            ],
            compiler_params=pltpu.CompilerParams(collective_id=0, has_side_effects=True, vmem_limit_bytes=64946176),
            name="sweeps",
        )(mat_rows, tele_rows, dang_rows.reshape(ROWS // 128, 128), damping, start_rows)

    return jax.shard_map(local_sweeps, mesh=mesh, in_specs=(spec_rows, spec_rows, spec_vec, P(None), spec_rows), out_specs=spec_rows, check_vma=False)
```

```python
import functools

import jax
import jax.numpy as jnp
from jax import lax
from jax.experimental import pallas as pl
from jax.experimental.pallas import tpu as pltpu
from jax.sharding import PartitionSpec as P

MESH = pl.DeviceIdType.MESH

DEV = 8
ROWS = 2048
TILE = 512
HALF = 128
COLS = 256
KEPT = (0, 1, 2, 3, 14, 15, 24, 25, 26, 27, 28, 29, 30, 31)
STREAMED = tuple(c for c in range(32) if c not in KEPT)
RING = 6
MROWS = 1024
SENT = 1024

X_SLOTS = ((0, 0, 0), (0, 2, 0), (0, 0, 1), (0, 2, 1), (0, 1, 2), (1, 1, 2), (1, 3, 0), (0, 3, 0), (1, 3, 1), (0, 3, 1))
Y_SLOTS = ((0, 1, 0), (0, 3, 0), (0, 1, 1), (0, 3, 1), (0, 0, 2), (1, 0, 2), (1, 2, 0), (0, 2, 0), (1, 2, 1), (0, 2, 1))


def kernel(sweeps, mat, tele, dang, damp, start, acc, factors, rbuf, abuf, tbuf, dcol, draw, mpair, mchip, asem, lsem, ssem, xsem, ysem, dsem, msem):
    me = lax.axis_index("row")
    core = lax.rem(me, 2)
    xbit = lax.rem(lax.div(me, 2), 2)
    ybit = lax.div(me, 4)

    def device(xb, yb, cb):
        return yb * 4 + xb * 2 + cb

    xn, yn, pt = device(1 - xbit, ybit, core), device(xbit, 1 - ybit, core), device(xbit, ybit, 1 - core)
    dg = device(1 - xbit, 1 - ybit, core)
    pxn, pyn, pdg = device(1 - xbit, ybit, 1 - core), device(xbit, 1 - ybit, 1 - core), device(1 - xbit, 1 - ybit, 1 - core)

    order = [(me, j) for j in range(4)] + [(pt, j) for j in range(4)]
    order += [(xn, 0), (xn, 2), (yn, 1), (yn, 3), (pxn, 0), (pxn, 2), (pyn, 1), (pyn, 3)]
    order += [(xn, 1), (yn, 0), (pxn, 1), (pyn, 0), (dg, 1), (dg, 0), (pdg, 1), (pdg, 0)]
    order += [(dg, 3), (dg, 2), (pdg, 3), (pdg, 2), (xn, 3), (yn, 2), (pxn, 3), (pyn, 2)]

    def first(dv, j):
        return pl.multiple_of(dv * ROWS + j * TILE, TILE)

    def slot_of(c):
        return KEPT.index(c) if c in KEPT else len(KEPT) + STREAMED.index(c) % RING

    def load(c):
        dv, j = order[c]
        return pltpu.make_async_copy(mat.at[:, pl.ds(first(dv, j), TILE)], abuf.at[slot_of(c)], asem.at[slot_of(c)])

    def piece(p, dv, j, h):
        return rbuf.at[p, slice(None) if h == 2 else h, pl.ds(first(dv, j), TILE), :]

    def send(p, dv, j, h, to, recv):
        return pltpu.make_async_remote_copy(
            src_ref=piece(p, dv, j, h), dst_ref=piece(p, dv, j, h), send_sem=ssem.at[p, h % 2], recv_sem=recv,
            device_id={"row": to}, device_id_type=MESH,
        )

    def arrived(p, dv, j, h, recv):
        pltpu.make_async_copy(piece(p, dv, j, h), piece(p, dv, j, h), recv).wait()

    def send_x(p, k):
        fwd, j, h = X_SLOTS[k]
        send(p, yn if fwd else me, j, h, xn, xsem.at[p, k]).start()

    def send_y(p, k):
        fwd, j, h = Y_SLOTS[k]
        send(p, xn if fwd else me, j, h, yn, ysem.at[p, k]).start()

    def share_own(p, j, h):
        send(p, me, j, h, pt, dsem.at[p, 2 * j + h]).start()

    def take(p, k):
        fwd, j, h = X_SLOTS[k]
        src = dg if fwd else xn
        arrived(p, src, j, h, xsem.at[p, k])
        send(p, src, j, h, pt, dsem.at[p, 8 + k]).start()
        fwd, j, h = Y_SLOTS[k]
        src = dg if fwd else yn
        arrived(p, src, j, h, ysem.at[p, k])
        send(p, src, j, h, pt, dsem.at[p, 18 + k]).start()

    def take_shared(p, ks):
        for k in ks:
            fwd, j, h = X_SLOTS[k]
            arrived(p, pdg if fwd else pxn, j, h, dsem.at[p, 8 + k])
            fwd, j, h = Y_SLOTS[k]
            arrived(p, pdg if fwd else pyn, j, h, dsem.at[p, 18 + k])

    def mass_of(values, rows, h):
        total = None
        for u in range(TILE // 128):
            line = rows.start // 128 + u
            part = values[u * 128:(u + 1) * 128] * dcol[:, line:line + 1]
            part = jnp.sum(part.reshape(-1, 8, HALF), axis=0)
            total = part if total is None else total + part
        return jnp.sum(total, axis=0, keepdims=True)

    def mass_copy(ref, sems, to):
        return pltpu.make_async_remote_copy(
            src_ref=ref[0], dst_ref=ref[1], send_sem=sems.at[0], recv_sem=sems.at[1], device_id={"row": to}, device_id_type=MESH
        )

    def send_mass(p):
        mass_copy((mpair.at[p, 0], mpair.at[p, 1]), msem.at[0, p], pt).start()

    chip = ybit * 2 + xbit

    def chip_mass(p):
        mass_copy((mpair.at[p, 0], mpair.at[p, 1]), msem.at[0, p], pt).wait()
        mchip[p, chip] = mpair[p, 0] + mpair[p, 1]

    def send_chip_mass(p):
        for to in (xn, yn, dg):
            mass_copy((mchip.at[p, chip], mchip.at[p, chip]), msem.at[1, p], to).start()

    def wait_a(t, cs):
        for c in cs:
            if c in KEPT:
                @pl.when(t == 0)
                def _():
                    load(c).wait()
            else:
                load(c).wait()

    def refill(t, cs):
        for c in cs:
            if c in KEPT:
                continue
            later = STREAMED.index(c) + RING
            if later < len(STREAMED):
                load(STREAMED[later]).start()
            else:
                @pl.when(t < sweeps - 1)
                def _():
                    load(STREAMED[later - len(STREAMED)]).start()

    def wide(p, c):
        r = pl.ds(first(*order[c]), TILE)
        return jnp.concatenate([rbuf[p, 0, r, :], rbuf[p, 1, r, :]], axis=1)

    def matmul(t, p, cs, init=False):
        wait_a(t, cs)

        for i in range(ROWS // MROWS):
            rows = pl.ds(i * MROWS, MROWS)
            total = None
            for c in cs:
                part = jnp.dot(abuf[slot_of(c), rows, :], wide(p, c), preferred_element_type=jnp.float32)
                total = part if total is None else total + part
            acc[rows, :] = total if init else acc[rows, :] + total

        refill(t, cs)

    def matmul_half(p, cs, h):
        for i in range(ROWS // MROWS):
            rows = pl.ds(i * MROWS, MROWS)
            lanes = pl.ds(h * HALF, HALF)
            total = None
            for c in cs:
                part = jnp.dot(abuf[slot_of(c), rows, :], rbuf[p, h, pl.ds(first(*order[c]), TILE), :], preferred_element_type=jnp.float32)
                total = part if total is None else total + part
            acc[rows, lanes] += total

    barrier = pltpu.get_barrier_semaphore()
    for dx, dy, dc in [(a, b, c) for a in range(2) for b in range(2) for c in range(2)][1:]:
        to = device(lax.rem(xbit + dx, 2), lax.rem(ybit + dy, 2), lax.rem(core + dc, 2))
        pl.semaphore_signal(barrier, inc=1, device_id={"row": to}, device_id_type=MESH)
    own_rows = []
    for j in range(4):
        rows = pl.ds(j * TILE, TILE)
        own_rows.append(pltpu.make_async_copy(start.at[rows, :], acc.at[rows, :], lsem.at[3 + j]))
        own_rows[j].start()
    own_dang = pltpu.make_async_copy(dang, draw, lsem.at[0])
    own_dang.start()
    own_damp = pltpu.make_async_copy(damp, factors, lsem.at[1])
    own_damp.start()
    for c in sorted(KEPT + STREAMED[:RING]):
        load(c).start()
    own_tele = pltpu.make_async_copy(tele, tbuf, lsem.at[2])
    own_tele.start()
    for j in range(4):
        own_rows[j].wait()
        for h in range(2):
            rbuf[0, h, pl.ds(first(me, j), TILE), :] = acc[pl.ds(j * TILE, TILE), pl.ds(h * HALF, HALF)].astype(jnp.bfloat16)
        if j == 1:
            pl.semaphore_wait(barrier, DEV - 1)
            send_x(0, 0)
            send_y(0, 0)
    for k in range(1, 5):
        send_x(0, k)
        send_y(0, k)
    for h in range(2):
        for j in range(4):
            share_own(0, j, h)
    own_dang.wait()
    lines = jnp.concatenate([draw[...].astype(jnp.float32), jnp.zeros((128 - ROWS // 128, 128), jnp.float32)], axis=0)
    dcol[...] = jnp.transpose(lines)
    for h in range(2):
        total = None
        for j in range(4):
            rows = pl.ds(j * TILE, TILE)
            part = mass_of(acc[rows, pl.ds(h * HALF, HALF)], rows, h)
            total = part if total is None else total + part
        mpair[0, 0, :, pl.ds(h * HALF, HALF)] = total
    own_tele.wait()
    own_damp.wait()

    @pl.loop(0, sweeps)
    def _(t):
        p = lax.rem(t, 2)
        q = 1 - p
        for j in range(4):
            for h in range(2):
                arrived(p, pt, j, h, dsem.at[p, 2 * j + h])
        send_mass(p)
        matmul(t, p, range(0, 8), init=True)
        chip_mass(p)
        for k in range(3):
            take(p, k)
        send_chip_mass(p)
        for k in (5, 6, 7):
            send_x(p, k)
            send_y(p, k)
        take(p, 3)
        for k in (8, 9):
            send_x(p, k)
            send_y(p, k)
        matmul(t, p, range(8, 12))
        take_shared(p, range(0, 4))
        matmul(t, p, range(12, 16))
        for s in range(2):
            take(p, 4 + s)
            matmul(t, p, range(16 + 4 * s, 18 + 4 * s))
            take_shared(p, (4 + s,))
            matmul(t, p, range(18 + 4 * s, 20 + 4 * s))
        wait_a(t, range(24, 32))
        others = mchip.at[p, pl.ds(0, 3)]
        pltpu.make_async_copy(others, others, msem.at[1, p, 1]).wait()
        pltpu.make_async_copy(others, others, msem.at[1, p, 0]).wait()
        mass = jnp.sum(mchip[p], axis=0)
        factor = factors[t]
        nodes = DEV * ROWS
        for h in range(2):
            take(p, 6 + 2 * h)
            matmul_half(p, (24, 25), h)
            take_shared(p, (6 + 2 * h,))
            matmul_half(p, (26, 27), h)
            take(p, 7 + 2 * h)
            matmul_half(p, (28, 29), h)
            take_shared(p, (7 + 2 * h,))
            lanes = pl.ds(h * HALF, HALF)
            row = (factor / nodes) * mass[:, h * HALF:(h + 1) * HALF]
            for i in range(ROWS // SENT):
                rows = pl.ds(i * SENT, SENT)
                parts = [jnp.dot(abuf[slot_of(c), rows, :], rbuf[p, h, pl.ds(first(*order[c]), TILE), :], preferred_element_type=jnp.float32) for c in (30, 31)]
                new = factor * (acc[rows, lanes] + parts[0]) + factor * parts[1] + (1.0 - factor) * tbuf[rows, lanes] + row
                acc[rows, lanes] = new
                rbuf[q, h, pl.ds(first(me, 2 * i), SENT), :] = new.astype(jnp.bfloat16)

                if i == ROWS // SENT - 1:
                    sent = rbuf.at[p, :, pl.ds(0, 18 * TILE), :] if h == 0 else rbuf.at[p, 1, pl.ds(0, 20 * TILE), :]
                    pltpu.make_async_copy(sent, sent, ssem.at[p, h]).wait()

                @pl.when(t < sweeps - 1)
                def _():
                    send_x(q, i + 2 * h)
                    send_y(q, i + 2 * h)
                    share_own(q, 2 * i, h)
                    share_own(q, 2 * i + 1, h)
                    if i + h == 2:
                        send_x(q, 4)
                        send_y(q, 4)


        @pl.when(t < sweeps - 1)
        def _():
            for h in range(2):
                lanes = pl.ds(h * HALF, HALF)
                held = None
                for j in range(4):
                    rows = pl.ds(j * TILE, TILE)
                    part = mass_of(acc[rows, lanes], rows, h)
                    held = part if held is None else held + part
                mpair[q, 0, :, lanes] = held


def solution(mesh):
    spec_rows = P(("batch", "row"), None)
    spec_vec = P(("batch", "row"))

    def local_sweeps(mat_rows, tele_rows, dang_rows, damping, start_rows):
        sweeps = damping.shape[0]
        hbm = pl.BlockSpec(memory_space=pl.ANY)
        return pl.pallas_call(
            functools.partial(kernel, sweeps),
            out_shape=pltpu.VMEM((ROWS, COLS), jnp.float32),
            in_specs=[hbm] * 5,
            out_specs=pl.BlockSpec(memory_space=pltpu.VMEM),
            scratch_shapes=[
                pltpu.SMEM((sweeps,), jnp.float32),
                pltpu.VMEM((2, 2, DEV * ROWS, HALF), jnp.bfloat16),
                pltpu.VMEM((len(KEPT) + RING, ROWS, TILE), jnp.bfloat16),
                pltpu.VMEM((ROWS, COLS), jnp.float32),
                pltpu.VMEM((128, 128), jnp.float32),
                pltpu.VMEM((ROWS // 128, 128), jnp.int32),
                pltpu.VMEM((2, 2, 1, COLS), jnp.float32),
                pltpu.VMEM((2, 4, 1, COLS), jnp.float32),
                pltpu.SemaphoreType.DMA((len(KEPT) + RING,)),
                pltpu.SemaphoreType.DMA((7,)),
                pltpu.SemaphoreType.DMA((2, 2)),
                pltpu.SemaphoreType.DMA((2, 10)),
                pltpu.SemaphoreType.DMA((2, 10)),
                pltpu.SemaphoreType.DMA((2, 28)),
                pltpu.SemaphoreType.DMA((2, 2, 2)),
            ],
            compiler_params=pltpu.CompilerParams(collective_id=0, has_side_effects=True, vmem_limit_bytes=64946176),
            name="sweeps",
        )(mat_rows, tele_rows, dang_rows.reshape(ROWS // 128, 128), damping, start_rows)

    return jax.shard_map(local_sweeps, mesh=mesh, in_specs=(spec_rows, spec_rows, spec_vec, P(None), spec_rows), out_specs=spec_rows, check_vma=False)
```
